32 devices in a mesh: dp: 4 (over y, z), sp: 8 (over x, core).
Axes of the slice: x: 4, y: 2, z: 2, core: 2. Of those that a mesh axis runs over, the one named last changes fastest.
The devices are a block of a 4x4x8 slice.
Arguments:
- images: bfloat16 [128, 32, 512, 64], P('dp', 'sp'), parts along dimension 0
- w_a: bfloat16 [1, 3, 3, 64, 64], replicated
- bn_a: float32 [1, 2, 64], replicated
- w_down: bfloat16 [3, 3, 64, 128], replicated
- bn_down: float32 [2, 128], replicated
- w_in: bfloat16 [3, 128, 128], replicated
- bn_in: float32 [3, 2, 128], replicated
- w_mid: bfloat16 [3, 3, 3, 128, 128], replicated
- bn_mid: float32 [3, 2, 128], replicated
- w_out: bfloat16 [3, 128, 128], replicated
- bn_out: float32 [3, 2, 128], replicated
Outputs:
- output: bfloat16 [128, 16, 256, 128], P('dp', 'sp'), parts along dimension 0
There are 4 independent parts. The reference program is written for one: setup_inputs(seed, part) draws one part's arguments, and reference() takes and returns one part's arrays. A program takes and returns all parts, laid end to end along the dimension named above; an argument that names none is the same for every part.
All inputs are finite; a program needn't handle non-finite values.
Results may differ from the reference program's by a relative error of at most 0.0193321.
Values are sent between devices in bfloat16 or wider.
A program may use at most 768 MiB of HBM per device.

```python
import jax
import jax.numpy as jnp
from jax import lax

IMAGES = 32
ROWS_DEV = 4
IMG_WIDTH = 512
LAYERS_A = 1
BLOCKS_B = 3
CHAN_A = 64
CHAN_MID = 128
CHAN_B = 128
GROUP_SIZE = 8
NORM_EPS = 1e-5
CONV_DIMS = ("NHWC", "HWIO", "NHWC")


def conv_weight(draw_key, full_shape, fan_in):
    return (jax.random.normal(draw_key, full_shape, jnp.float32) * fan_in ** -0.5).astype(jnp.bfloat16)


def norm_params(draw_key, lead_dims, chan_count):
    key_gain, key_shift = jax.random.split(draw_key)
    norm_gain = jax.random.uniform(key_gain, lead_dims + (chan_count,), jnp.float32, 0.6, 1.4)
    norm_shift = 0.4 * jax.random.normal(key_shift, lead_dims + (chan_count,), jnp.float32)
    return jnp.stack([norm_gain, norm_shift], axis=-2)


def setup_inputs(seed: int = 0, part: int = 0) -> dict:
    base_key = jax.random.key(seed)
    part_key = jax.random.fold_in(base_key, part)
    key_noise, key_amp, key_phase = jax.random.split(part_key, 3)
    weight_keys = jax.random.split(base_key, 10)
    height = GROUP_SIZE * ROWS_DEV
    row_pos = (jnp.arange(height, dtype=jnp.float32) + 0.5) / height
    band_amp = 1.5 * jax.random.normal(key_amp, (CHAN_A,), jnp.float32)
    band_phase = 6.2832 * jax.random.uniform(key_phase, (CHAN_A,), jnp.float32)
    row_band = band_amp * (1.0 - 2.0 * row_pos)[:, None] + jnp.sin(12.566 * row_pos[:, None] + band_phase)
    pixel_noise = jax.random.normal(key_noise, (IMAGES, height, IMG_WIDTH, CHAN_A), jnp.float32)
    return {
        "images": (pixel_noise + row_band[None, :, None, :]).astype(jnp.bfloat16),
        "w_a": conv_weight(weight_keys[0], (LAYERS_A, 3, 3, CHAN_A, CHAN_A), 9 * CHAN_A),
        "bn_a": norm_params(weight_keys[1], (LAYERS_A,), CHAN_A),
        "w_down": conv_weight(weight_keys[2], (3, 3, CHAN_A, CHAN_B), 9 * CHAN_A),
        "bn_down": norm_params(weight_keys[3], (), CHAN_B),
        "w_in": conv_weight(weight_keys[4], (BLOCKS_B, CHAN_B, CHAN_MID), CHAN_B),
        "bn_in": norm_params(weight_keys[5], (BLOCKS_B,), CHAN_MID),
        "w_mid": conv_weight(weight_keys[6], (BLOCKS_B, 3, 3, CHAN_MID, CHAN_MID), 9 * CHAN_MID),
        "bn_mid": norm_params(weight_keys[7], (BLOCKS_B,), CHAN_MID),
        "w_out": conv_weight(weight_keys[8], (BLOCKS_B, CHAN_MID, CHAN_B), CHAN_MID),
        "bn_out": norm_params(weight_keys[9], (BLOCKS_B,), CHAN_B),
    }


def conv_full(hidden, weight, stride):
    return lax.conv_general_dilated(hidden.astype(jnp.float32), weight.astype(jnp.float32), (stride, stride), "SAME", dimension_numbers=CONV_DIMS)


def conv_point(hidden, weight):
    return jnp.einsum("bhwc,cd->bhwd", hidden.astype(jnp.float32), weight.astype(jnp.float32))


def batch_norm(pre_act, params):
    chan_mean = jnp.mean(pre_act, axis=(0, 1, 2))
    chan_var = jnp.mean(pre_act * pre_act, axis=(0, 1, 2)) - chan_mean * chan_mean
    chan_scale = params[0] * lax.rsqrt(chan_var + NORM_EPS)
    return (pre_act - chan_mean) * chan_scale + params[1]


def norm_relu(pre_act, params):
    return jax.nn.relu(batch_norm(pre_act, params)).astype(jnp.bfloat16)


def reference(images, w_a, bn_a, w_down, bn_down, w_in, bn_in, w_mid, bn_mid, w_out, bn_out):
    def stage_a(hidden, layer_args):
        return norm_relu(conv_full(hidden, layer_args[0], 1), layer_args[1]), None

    def bottleneck(hidden, block_args):
        w_first, bn_first, w_three, bn_three, w_last, bn_last = block_args
        branch = norm_relu(conv_point(hidden, w_first), bn_first)
        branch = norm_relu(conv_full(branch, w_three, 1), bn_three)
        summed = batch_norm(conv_point(branch, w_last), bn_last) + hidden.astype(jnp.float32)
        return jax.nn.relu(summed).astype(jnp.bfloat16), None

    hidden, _ = lax.scan(stage_a, images, (w_a, bn_a))
    hidden = norm_relu(conv_full(hidden, w_down, 2), bn_down)
    hidden, _ = lax.scan(bottleneck, hidden, (w_in, bn_in, w_mid, bn_mid, w_out, bn_out))
    return hidden
```

```python
import functools

import jax
import jax.numpy as jnp
from jax import lax
from jax.experimental import pallas as pl
from jax.experimental.pallas import tpu as pltpu
from jax.sharding import PartitionSpec as P

NORM_EPS = 1e-5
BF = jnp.bfloat16
F32 = jnp.float32
OPP_CORE = 0
GROUP = 4
SLOTS = 4


def cat(parts, axis):
    return jnp.concatenate(parts, axis=axis)


def banded(taps, rows_in, rows_out, stride, first):
    zero = jnp.zeros_like(taps[0])
    rows = []
    for ri in rows_in:
        cols = []
        for ro in rows_out:
            dy = ri + first - stride * ro
            cols.append(taps[dy] if 0 <= dy < len(taps) else zero)
        rows.append(cat(cols, 1))
    return cat(rows, 0)


def pack_weights(w_a, w_down, w_in, w_mid, w_out):
    blocks = w_in.shape[0]
    wa, w4, wdn, wdh = [], [], [], []
    for dx in range(3):
        ta = [w_a[0, dy, dx] for dy in range(3)]
        zero = jnp.zeros_like(ta[0])
        wa.append(banded(ta, range(6), range(4), 1, 0))
        w4.append(cat([cat([t, zero], 1) for t in ta + [zero]], 0))
        td = [w_down[dy, dx] for dy in range(3)]
        wdn.append(banded(td, range(4), range(2), 2, 0))
        wdh.append(banded(td + [jnp.zeros_like(td[0])], (4, 5), (0, 1), 2, 0))
    wa, w4, wd = cat(wa, 0), cat(w4, 0), cat(wdn + wdh, 0)

    def diag(w):
        z = jnp.zeros_like(w)
        return cat([cat([w, z], 1), cat([z, w], 1)], 0)

    w_in2 = jnp.stack([diag(w_in[j]) for j in range(blocks)])
    w_out2 = jnp.stack([diag(w_out[j]) for j in range(blocks)])
    loc, halo = [], []
    for j in range(blocks):
        ml, mh = [], []
        for dx in range(3):
            tm = [w_mid[j, dy, dx] for dy in range(3)]
            z = jnp.zeros_like(tm[0])
            ml.append(banded(tm, (0, 1), (0, 1), 1, 1))
            mh.append(cat([cat([tm[0], z], 1), cat([z, tm[2]], 1)], 0))
        loc.append(cat(ml, 0))
        halo.append(cat(mh, 0))
    return wa, w4, wd, w_in2, w_out2, jnp.stack(loc), jnp.stack(halo)


def body(
    dims, img, wa, w4, wd, w_in, w_out, w_loc, w_halo, bn, out,
    xb, halo, xs, za, z4, zb, hb, ub, hh, rb,
    msg, pslot, cmsg, slots,
    ld_sem, im_send, im_recv, ex_send, ex_recv, ar_send, ar_recv, out_sem,
):
    n_img, width, sp_n, blocks, count_a, count_b = dims
    half = width // 2
    n_grp = n_img // GROUP
    rows = GROUP * half
    me = lax.axis_index("sp")
    core = lax.rem(me, 2)
    chip = lax.div(me, 2)
    chips = sp_n // 2
    has_up = me > 0
    has_dn = me < sp_n - 1
    up = jnp.maximum(me - 1, 0)
    dn = jnp.minimum(me + 1, sp_n - 1)

    def remote(src, dst, ssem, rsem, dev):
        return pltpu.make_async_remote_copy(
            src_ref=src, dst_ref=dst, send_sem=ssem, recv_sem=rsem,
            device_id={"sp": dev}, device_id_type=pl.DeviceIdType.MESH)

    bar = pltpu.get_barrier_semaphore()
    for k in range(1, sp_n):
        pl.semaphore_signal(bar, inc=1, device_id={"sp": lax.rem(me + k, sp_n)}, device_id_type=pl.DeviceIdType.MESH)
    pl.semaphore_wait(bar, sp_n - 1)

    def img_copy(slot, g, dev):
        row = (3, 0, 1)[slot]
        part = pl.ds(g * GROUP, GROUP)
        return remote(img.at[part, row], halo.at[slot, part], im_send.at[slot, g], im_recv.at[slot, g], dev)

    @pl.loop(0, n_grp)
    def _(g):
        @pl.when(has_dn)
        def _():
            img_copy(0, g, dn).start()

        @pl.when(has_up)
        def _():
            img_copy(1, g, up).start()

    @pl.when(has_up)
    def _():
        @pl.loop(0, n_grp)
        def _(g):
            img_copy(2, g, up).start()

    @pl.when(jnp.logical_not(has_up))
    def _():
        @pl.loop(0, n_img)
        def _(n):
            halo[0, n] = jnp.zeros(halo.shape[2:], BF)
            hh[0, n] = jnp.zeros(hh.shape[2:], BF)
            rb[0, n] = jnp.zeros(rb.shape[2:], BF)

    @pl.when(jnp.logical_not(has_dn))
    def _():
        @pl.loop(0, n_img)
        def _(n):
            halo[1, n] = jnp.zeros(halo.shape[2:], BF)
            halo[2, n] = jnp.zeros(halo.shape[2:], BF)
            hh[1, n] = jnp.zeros(hh.shape[2:], BF)
            rb[1, n] = jnp.zeros(rb.shape[2:], BF)

    def dot(a, b):
        return jnp.dot(a, b, preferred_element_type=F32)

    def add_stats(carry, z):
        s, q = carry
        zz = z.reshape(z.shape[0] // 8, 8, z.shape[1])
        return s + jnp.sum(zz, axis=0), q + jnp.sum(zz * zz, axis=0)

    zero_stats = (jnp.zeros((8, 256), F32), jnp.zeros((8, 256), F32))

    def norm(z, m):
        return jnp.maximum((z - m[0]) * m[1] + m[2], 0.0)

    def moments(k, stats, count, fold64):
        s, q = (t[:, :128] + t[:, 128:] for t in stats)
        if fold64:
            s, q = s + pltpu.roll(s, 64, 1), q + pltpu.roll(q, 64, 1)
        own = cat([s, q], 0)
        msg[k] = own
        first = remote(msg.at[k], pslot.at[k], ar_send.at[k, 0], ar_recv.at[k, 3], me + 1 - 2 * core)
        first.start()
        first.wait_recv()
        mine = own + pslot[k]
        cmsg[k] = mine
        near = lax.rem(chip + 1 + core * (chips - 2), chips)
        far = lax.rem(chip + 2, chips)
        for c in range(2):
            remote(cmsg.at[k], slots.at[k, core], ar_send.at[k, 1 + c], ar_recv.at[k, core], near * 2 + c).start()

        @pl.when(core == OPP_CORE)
        def _():
            for c in range(2):
                remote(cmsg.at[k], slots.at[k, 2], ar_send.at[k, 3 + c], ar_recv.at[k, 2], far * 2 + c).start()

        for c in range(3):
            remote(cmsg.at[k], slots.at[k, c], ar_send.at[k, 1], ar_recv.at[k, c], me).wait_recv()
        tot = (mine + slots[k, 2]) + (slots[k, 0] + slots[k, 1])
        inv = 1.0 / count
        mean = jnp.sum(tot[:8], axis=0, keepdims=True) * inv
        var = jnp.sum(tot[8:], axis=0, keepdims=True) * inv - mean * mean
        p = bn[k]
        scale = p[0:1] * lax.rsqrt(var + NORM_EPS)
        return tuple(cat([t, t], 1) for t in (mean, scale, p[1:2]))

    def shifts(u):
        row = lax.rem(lax.broadcasted_iota(jnp.int32, (u.shape[0], 1), 0), half)
        zero = jnp.zeros_like(u)
        prev = jnp.where(row == 0, zero, pltpu.roll(u, 1, 0))
        nxt = jnp.where(row == half - 1, zero, pltpu.roll(u, u.shape[0] - 1, 0))
        return cat([prev, u, nxt], 1)

    def shifts_w(u):
        row = lax.broadcasted_iota(jnp.int32, (u.shape[0], 1), 0)
        zero = jnp.zeros_like(u)
        prev = jnp.where(row == 0, zero, pltpu.roll(u, 1, 0))
        nxt = jnp.where(row == u.shape[0] - 1, zero, pltpu.roll(u, u.shape[0] - 1, 0))
        return cat([prev, u, nxt], 1)

    def load(n):
        slot = lax.rem(n, SLOTS)
        return pltpu.make_async_copy(img.at[n], xb.at[slot], ld_sem.at[slot])

    for n in range(SLOTS - 1):
        load(n).start()

    def stage_a(g, carry):
        @pl.when(has_up)
        def _():
            img_copy(0, g, dn).wait_recv()

        @pl.when(has_dn)
        def _():
            img_copy(1, g, up).wait_recv()

        def one(i, carry):
            n = g * GROUP + i

            @pl.when(n + SLOTS - 1 < n_img)
            def _():
                load(n + SLOTS - 1).start()

            load(n).wait()
            x = xb.at[lax.rem(n, SLOTS)]
            t0 = cat([halo[0, n], x[0]], 0).T
            t1 = cat([x[1], x[2]], 0).T
            t2 = cat([x[3], halo[1, n]], 0).T
            xs[n] = t2
            z = dot(shifts_w(cat([t0, t1, t2], 1)), wa[...])
            za[0, n] = z[:, :128]
            za[1, n] = z[:, 128:]
            return add_stats(carry, z)

        return lax.fori_loop(0, GROUP, one, carry)

    m = moments(0, lax.fori_loop(0, n_grp, stage_a, zero_stats), count_a, True)
    m_half = tuple(t[:, :128] for t in m)

    def stage_d(g, carry):
        @pl.when(has_dn)
        def _():
            img_copy(2, g, up).wait_recv()

        def one(i, carry):
            n = g * GROUP + i
            t3 = cat([halo[2, n], halo[2, n]], 0).T
            z4[...] = dot(shifts_w(cat([xs[n], t3], 1)), w4[...])
            ev, od = pl.ds(0, half, stride=2), pl.ds(1, half, stride=2)
            e = norm(cat([za[0, n, ev, :], za[1, n, ev, :]], 1), m).astype(BF)
            o = norm(cat([za[0, n, od, :], za[1, n, od, :]], 1), m).astype(BF)
            e4 = jnp.where(has_dn, norm(z4[ev, :], m_half), 0.0).astype(BF)
            o4 = jnp.where(has_dn, norm(z4[od, :], m_half), 0.0).astype(BF)
            row = lax.broadcasted_iota(jnp.int32, (half, 1), 0)

            def nxt(t):
                return jnp.where(row == half - 1, jnp.zeros_like(t), pltpu.roll(t, half - 1, 0))

            z = dot(cat([e, o, nxt(e), e4, o4, nxt(e4)], 1), wd[...])
            zb[n] = z
            return add_stats(carry, z)

        return lax.fori_loop(0, GROUP, one, carry)

    m = moments(1, lax.fori_loop(0, n_grp, stage_d, zero_stats), count_b, False)

    def ex_copy(slot, g, src, dst, dev):
        part = pl.ds(g * GROUP, GROUP)
        return remote(src.at[1 - slot, part], dst.at[slot, part], ex_send.at[slot, g], ex_recv.at[slot, g], dev)

    def ex_start(g, src, dst):
        @pl.when(has_dn)
        def _():
            ex_copy(0, g, src, dst, dn).start()

        @pl.when(has_up)
        def _():
            ex_copy(1, g, src, dst, up).start()

    def ex_wait_send(src, dst):
        @pl.loop(0, n_grp)
        def _(g):
            @pl.when(has_dn)
            def _():
                ex_copy(0, g, src, dst, dn).wait_send()

            @pl.when(has_up)
            def _():
                ex_copy(1, g, src, dst, up).wait_send()

    def get(ref, part):
        return cat([ref[0, part].reshape(rows, 128), ref[1, part].reshape(rows, 128)], 1)

    def put(ref, part, v):
        ref[0, part] = v[:, :128].reshape(GROUP, half, 128)
        ref[1, part] = v[:, 128:].reshape(GROUP, half, 128)

    lane = lax.broadcasted_iota(jnp.int32, (1, 256), 1)
    valid = ((lane < 128) & has_up) | ((lane >= 128) & has_dn)

    for j in range(blocks):
        m_prev = m
        src, dst = (hb, hh) if j == 0 else (ub, rb)

        def conv_in(g, carry):
            part = pl.ds(g * GROUP, GROUP)
            z = zb[part].reshape(rows, 256)
            if j == 0:
                h = norm(z, m_prev).astype(BF)
            else:
                h = jnp.maximum((z - m_prev[0]) * m_prev[1] + m_prev[2] + get(hb, part).astype(F32), 0.0).astype(BF)
            put(hb, part, h)
            if j == 0:
                @pl.when(g > 0)
                def _():
                    ex_start(g - 1, src, dst)
            z = dot(h, w_in[j])
            zb[part] = z.reshape(GROUP, half, 256)
            return add_stats(carry, z)

        stats = lax.fori_loop(0, n_grp, conv_in, zero_stats)
        if j == 0:
            ex_start(n_grp - 1, src, dst)
        m_in = moments(2 + 3 * j, stats, count_b, False)

        def mid_local(g, carry):
            part = pl.ds(g * GROUP, GROUP)
            u = norm(zb[part].reshape(rows, 256), m_in).astype(BF)
            zb[part] = dot(shifts(u), w_loc[j]).reshape(GROUP, half, 256)
            return carry

        lax.fori_loop(0, n_grp, mid_local, 0)

        def mid_halo(g, carry):
            part = pl.ds(g * GROUP, GROUP)

            @pl.when(has_up)
            def _():
                ex_copy(0, g, src, dst, dn).wait_recv()

            @pl.when(has_dn)
            def _():
                ex_copy(1, g, src, dst, up).wait_recv()

            h = get(hh, part)
            if j > 0:
                z = dot(get(rb, part), w_out[j - 1])
                h = jnp.maximum((z - m_prev[0]) * m_prev[1] + m_prev[2] + h.astype(F32), 0.0).astype(BF)
                if j < blocks - 1:
                    put(hh, part, h)
            u = jnp.where(valid, norm(dot(h, w_in[j]), m_in), 0.0).astype(BF)
            z = zb[part].reshape(rows, 256) + dot(shifts(u), w_halo[j])
            zb[part] = z.reshape(GROUP, half, 256)
            return add_stats(carry, z)

        stats = lax.fori_loop(0, n_grp, mid_halo, zero_stats)
        ex_wait_send(src, dst)
        m_mid = moments(3 + 3 * j, stats, count_b, False)

        def conv_out(g, carry):
            part = pl.ds(g * GROUP, GROUP)
            u = norm(zb[part].reshape(rows, 256), m_mid).astype(BF)
            if j < blocks - 1:
                put(ub, part, u)

                @pl.when(g > 0)
                def _():
                    ex_start(g - 1, ub, rb)
            z = dot(u, w_out[j])
            zb[part] = z.reshape(GROUP, half, 256)
            return add_stats(carry, z)

        stats = lax.fori_loop(0, n_grp, conv_out, zero_stats)
        if j < blocks - 1:
            ex_start(n_grp - 1, ub, rb)
        m = moments(4 + 3 * j, stats, count_b, False)

    def out_copy(g, r):
        part = pl.ds(g * GROUP, GROUP)
        return pltpu.make_async_copy(hb.at[r, part], out.at[part, r], out_sem.at[r, g])

    def finish(g, carry):
        part = pl.ds(g * GROUP, GROUP)
        z = zb[part].reshape(rows, 256)
        h = jnp.maximum((z - m[0]) * m[1] + m[2] + get(hb, part).astype(F32), 0.0).astype(BF)
        put(hb, part, h)
        for r in range(2):
            out_copy(g, r).start()
        return carry

    lax.fori_loop(0, n_grp, finish, 0)

    @pl.loop(0, n_grp)
    def _(g):
        for r in range(2):
            out_copy(g, r).wait()

        @pl.when(has_dn)
        def _():
            img_copy(0, g, dn).wait_send()

        @pl.when(has_up)
        def _():
            img_copy(1, g, up).wait_send()
            img_copy(2, g, up).wait_send()

    @pl.loop(0, 2 + 3 * blocks)
    def _(k):
        remote(msg.at[k], pslot.at[k], ar_send.at[k, 0], ar_recv.at[k, 3], me).wait_send()
        for c in range(2):
            remote(cmsg.at[k], slots.at[k, 0], ar_send.at[k, 1 + c], ar_recv.at[k, 0], me).wait_send()

        @pl.when(core == OPP_CORE)
        def _():
            for c in range(2):
                remote(cmsg.at[k], slots.at[k, 2], ar_send.at[k, 3 + c], ar_recv.at[k, 2], me).wait_send()


def solution(mesh):
    sp_n = mesh.shape["sp"]

    def forward(images, w_a, bn_a, w_down, bn_down, w_in, bn_in, w_mid, bn_mid, w_out, bn_out):
        n_img, rows_dev, width, chan = images.shape
        half = width // 2
        blocks = w_in.shape[0]
        n_bn = 2 + 3 * blocks
        n_grp = n_img // GROUP
        packed = pack_weights(w_a, w_down, w_in, w_mid, w_out)
        rest = jnp.stack([bn_in, bn_mid, bn_out], axis=1).reshape(3 * blocks, 2, 128)
        bn = cat([jnp.tile(bn_a, (1, 1, 2)), bn_down[None], rest], 0)
        x = jnp.transpose(images, (0, 1, 3, 2))
        dims = (n_img, width, sp_n, blocks, n_img * rows_dev * width * sp_n, n_img * (rows_dev // 2) * half * sp_n)
        vmem = pl.BlockSpec(memory_space=pltpu.VMEM)
        anys = pl.BlockSpec(memory_space=pl.ANY)
        plane = (2, n_img, half, 128)
        return pl.pallas_call(
            functools.partial(body, dims),
            out_shape=jax.ShapeDtypeStruct((n_img, rows_dev // 2, half, 128), BF),
            in_specs=[anys] + [vmem] * 8,
            out_specs=anys,
            scratch_shapes=[
                pltpu.VMEM((SLOTS, rows_dev, chan, width), BF),
                pltpu.VMEM((3, n_img, chan, width), BF),
                pltpu.VMEM((n_img, width, 128), BF),
                pltpu.VMEM((2, n_img, width, 128), F32),
                pltpu.VMEM((width, 128), F32),
                pltpu.VMEM((n_img, half, 256), F32),
                pltpu.VMEM(plane, BF),
                pltpu.VMEM(plane, BF),
                pltpu.VMEM(plane, BF),
                pltpu.VMEM(plane, BF),
                pltpu.VMEM((n_bn, 16, 128), F32),
                pltpu.VMEM((n_bn, 16, 128), F32),
                pltpu.VMEM((n_bn, 16, 128), F32),
                pltpu.VMEM((n_bn, 3, 16, 128), F32),
                pltpu.SemaphoreType.DMA((SLOTS,)),
                pltpu.SemaphoreType.DMA((3, n_grp)),
                pltpu.SemaphoreType.DMA((3, n_grp)),
                pltpu.SemaphoreType.DMA((2, n_grp)),
                pltpu.SemaphoreType.DMA((2, n_grp)),
                pltpu.SemaphoreType.DMA((n_bn, 5)),
                pltpu.SemaphoreType.DMA((n_bn, 4)),
                pltpu.SemaphoreType.DMA((2, n_grp)),
            ],
            compiler_params=pltpu.CompilerParams(
                collective_id=0, has_side_effects=True, vmem_limit_bytes=67043328),
            name="stack",
        )(x, *packed, bn)

    act_spec = P("dp", "sp", None, None)
    return jax.shard_map(forward, mesh=mesh, in_specs=(act_spec,) + (P(),) * 10, out_specs=act_spec, check_vma=False)
```

```python
import functools

import jax
import jax.numpy as jnp
from jax import lax
from jax.experimental import pallas as pl
from jax.experimental.pallas import tpu as pltpu
from jax.sharding import PartitionSpec as P

NORM_EPS = 1e-5
BF = jnp.bfloat16
F32 = jnp.float32
OPP_CORE = 0
GROUP = 4
SLOTS = 4


def cat(parts, axis):
    return jnp.concatenate(parts, axis=axis)


def banded(taps, rows_in, rows_out, stride, first):
    zero = jnp.zeros_like(taps[0])
    rows = []
    for ri in rows_in:
        cols = []
        for ro in rows_out:
            dy = ri + first - stride * ro
            cols.append(taps[dy] if 0 <= dy < len(taps) else zero)
        rows.append(cat(cols, 1))
    return cat(rows, 0)


def pack_stage_a(w_a, w_down, wa, w4, wd):
    for dx in range(3):
        ta = [w_a[0, dy, dx] for dy in range(3)]
        zero = jnp.zeros_like(ta[0])
        wa[pl.ds(dx * 384, 384)] = banded(ta, range(6), range(4), 1, 0)
        w4[pl.ds(dx * 256, 256)] = cat([cat([t, zero], 1) for t in ta + [zero]], 0)
        td = [w_down[dy, dx] for dy in range(3)]
        wd[pl.ds(dx * 256, 256)] = banded(td, range(4), range(2), 2, 0)
        wd[pl.ds(768 + dx * 128, 128)] = banded(td + [jnp.zeros_like(td[0])], (4, 5), (0, 1), 2, 0)


def pack_stage_b(w_in, w_mid, w_out, in2, out2, loc, halo):
    def diag(a, b):
        z = jnp.zeros_like(a)
        return cat([cat([a, z], 1), cat([z, b], 1)], 0)

    for j in range(w_in.shape[0]):
        in2[j] = diag(w_in[j], w_in[j])
        out2[j] = diag(w_out[j], w_out[j])
        for dx in range(3):
            tm = [w_mid[j, dy, dx] for dy in range(3)]
            loc[j, pl.ds(dx * 256, 256)] = banded(tm, (0, 1), (0, 1), 1, 1)
            halo[j, pl.ds(dx * 256, 256)] = diag(tm[0], tm[2])


def body(
    dims, img, w_a_hbm, w_down_hbm, w_in_hbm, w_mid_hbm, w_out_hbm, bn_a, bn_down, bn_in, bn_mid, bn_out, out,
    w_a_raw, w_down_raw, w_in_raw, w_mid_raw, w_out_raw, wa, w4, wd, w_in, w_out, w_loc, w_halo,
    xb, halo, xs, za, z4, zb, hb, ub, hh, rb,
    msg, pslot, cmsg, slots,
    ld_sem, im_send, im_recv, ex_send, ex_recv, ar_send, ar_recv, out_sem, w_sem,
):
    n_img, width, sp_n, blocks, count_a, count_b = dims
    half = width // 2
    n_grp = n_img // GROUP
    rows = GROUP * half
    me = lax.axis_index("sp")
    core = lax.rem(me, 2)
    chip = lax.div(me, 2)
    chips = sp_n // 2
    has_up = me > 0
    has_dn = me < sp_n - 1
    up = jnp.maximum(me - 1, 0)
    dn = jnp.minimum(me + 1, sp_n - 1)

    def remote(src, dst, ssem, rsem, dev):
        return pltpu.make_async_remote_copy(
            src_ref=src, dst_ref=dst, send_sem=ssem, recv_sem=rsem,
            device_id={"sp": dev}, device_id_type=pl.DeviceIdType.MESH)

    w_copies = [
        pltpu.make_async_copy(src, dst, w_sem.at[i]) for i, (src, dst) in enumerate((
            (w_a_hbm, w_a_raw), (w_down_hbm, w_down_raw), (w_in_hbm, w_in_raw), (w_mid_hbm, w_mid_raw), (w_out_hbm, w_out_raw)))]
    for copy in w_copies:
        copy.start()

    def load(n):
        slot = lax.rem(n, SLOTS)
        return pltpu.make_async_copy(img.at[n], xb.at[slot], ld_sem.at[slot])

    for n in range(SLOTS - 1):
        load(n).start()

    bar = pltpu.get_barrier_semaphore()
    for k in range(1, sp_n):
        pl.semaphore_signal(bar, inc=1, device_id={"sp": lax.rem(me + k, sp_n)}, device_id_type=pl.DeviceIdType.MESH)
    pl.semaphore_wait(bar, sp_n - 1)

    def img_copy(slot, g, dev):
        row = (3, 0, 1)[slot]
        part = pl.ds(g * GROUP, GROUP)
        return remote(img.at[part, row], halo.at[slot, part], im_send.at[slot, g], im_recv.at[slot, g], dev)

    @pl.loop(0, n_grp)
    def _(g):
        @pl.when(has_dn)
        def _():
            img_copy(0, g, dn).start()

        @pl.when(has_up)
        def _():
            img_copy(1, g, up).start()

    @pl.when(has_up)
    def _():
        @pl.loop(0, n_grp)
        def _(g):
            img_copy(2, g, up).start()

    @pl.when(jnp.logical_not(has_up))
    def _():
        @pl.loop(0, n_img)
        def _(n):
            halo[0, n] = jnp.zeros(halo.shape[2:], BF)
            hh[0, n] = jnp.zeros(hh.shape[2:], BF)
            rb[0, n] = jnp.zeros(rb.shape[2:], BF)

    @pl.when(jnp.logical_not(has_dn))
    def _():
        @pl.loop(0, n_img)
        def _(n):
            halo[1, n] = jnp.zeros(halo.shape[2:], BF)
            halo[2, n] = jnp.zeros(halo.shape[2:], BF)
            hh[1, n] = jnp.zeros(hh.shape[2:], BF)
            rb[1, n] = jnp.zeros(rb.shape[2:], BF)

    def dot(a, b):
        return jnp.dot(a, b, preferred_element_type=F32)

    def add_stats(carry, z):
        s, q = carry
        zz = z.reshape(z.shape[0] // 8, 8, z.shape[1])
        return s + jnp.sum(zz, axis=0), q + jnp.sum(zz * zz, axis=0)

    zero_stats = (jnp.zeros((8, 256), F32), jnp.zeros((8, 256), F32))

    def norm(z, m):
        return jnp.maximum((z - m[0]) * m[1] + m[2], 0.0)

    def moments(k, stats, count, p, fold64=False):
        s, q = (t[:, :128] + t[:, 128:] for t in stats)
        if fold64:
            s, q = s + pltpu.roll(s, 64, 1), q + pltpu.roll(q, 64, 1)
        own = cat([s, q], 0)
        msg[k] = own
        first = remote(msg.at[k], pslot.at[k], ar_send.at[k, 0], ar_recv.at[k, 3], me + 1 - 2 * core)
        first.start()
        first.wait_recv()
        mine = own + pslot[k]
        cmsg[k] = mine
        near = lax.rem(chip + 1 + core * (chips - 2), chips)
        far = lax.rem(chip + 2, chips)
        for c in range(2):
            remote(cmsg.at[k], slots.at[k, core], ar_send.at[k, 1 + c], ar_recv.at[k, core], near * 2 + c).start()

        @pl.when(core == OPP_CORE)
        def _():
            for c in range(2):
                remote(cmsg.at[k], slots.at[k, 2], ar_send.at[k, 3 + c], ar_recv.at[k, 2], far * 2 + c).start()

        for c in range(3):
            remote(cmsg.at[k], slots.at[k, c], ar_send.at[k, 1], ar_recv.at[k, c], me).wait_recv()
        tot = (mine + slots[k, 2]) + (slots[k, 0] + slots[k, 1])
        inv = 1.0 / count
        mean = jnp.sum(tot[:8], axis=0, keepdims=True) * inv
        var = jnp.sum(tot[8:], axis=0, keepdims=True) * inv - mean * mean
        scale = p[0:1] * lax.rsqrt(var + NORM_EPS)
        return tuple(cat([t, t], 1) for t in (mean, scale, p[1:2]))

    def shifts(u):
        row = lax.rem(lax.broadcasted_iota(jnp.int32, (u.shape[0], 1), 0), half)
        zero = jnp.zeros_like(u)
        prev = jnp.where(row == 0, zero, pltpu.roll(u, 1, 0))
        nxt = jnp.where(row == half - 1, zero, pltpu.roll(u, u.shape[0] - 1, 0))
        return cat([prev, u, nxt], 1)

    def shifts_w(u):
        row = lax.broadcasted_iota(jnp.int32, (u.shape[0], 1), 0)
        zero = jnp.zeros_like(u)
        prev = jnp.where(row == 0, zero, pltpu.roll(u, 1, 0))
        nxt = jnp.where(row == u.shape[0] - 1, zero, pltpu.roll(u, u.shape[0] - 1, 0))
        return cat([prev, u, nxt], 1)

    for copy in w_copies:
        copy.wait()
    pack_stage_a(w_a_raw, w_down_raw, wa, w4, wd)
    pack_stage_b(w_in_raw, w_mid_raw, w_out_raw, w_in, w_out, w_loc, w_halo)

    def stage_a(g, carry):
        @pl.when(has_up)
        def _():
            img_copy(0, g, dn).wait_recv()

        @pl.when(has_dn)
        def _():
            img_copy(1, g, up).wait_recv()

        def one(i, carry):
            n = g * GROUP + i

            @pl.when(n + SLOTS - 1 < n_img)
            def _():
                load(n + SLOTS - 1).start()

            load(n).wait()
            x = xb.at[lax.rem(n, SLOTS)]
            t0 = cat([halo[0, n], x[0]], 0).T
            t1 = cat([x[1], x[2]], 0).T
            t2 = cat([x[3], halo[1, n]], 0).T
            xs[n] = t2
            z = dot(shifts_w(cat([t0, t1, t2], 1)), wa[...])
            za[0, n] = z[:, :128]
            za[1, n] = z[:, 128:]
            return add_stats(carry, z)

        return lax.fori_loop(0, GROUP, one, carry)

    m = moments(0, lax.fori_loop(0, n_grp, stage_a, zero_stats), count_a, cat([bn_a[0], bn_a[0]], 1), True)
    m_half = tuple(t[:, :128] for t in m)

    def stage_d(g, carry):
        @pl.when(has_dn)
        def _():
            img_copy(2, g, up).wait_recv()

        def one(i, carry):
            n = g * GROUP + i
            t3 = cat([halo[2, n], halo[2, n]], 0).T
            z4[...] = dot(shifts_w(cat([xs[n], t3], 1)), w4[...])
            ev, od = pl.ds(0, half, stride=2), pl.ds(1, half, stride=2)
            e = norm(cat([za[0, n, ev, :], za[1, n, ev, :]], 1), m).astype(BF)
            o = norm(cat([za[0, n, od, :], za[1, n, od, :]], 1), m).astype(BF)
            e4 = jnp.where(has_dn, norm(z4[ev, :], m_half), 0.0).astype(BF)
            o4 = jnp.where(has_dn, norm(z4[od, :], m_half), 0.0).astype(BF)
            row = lax.broadcasted_iota(jnp.int32, (half, 1), 0)

            def nxt(t):
                return jnp.where(row == half - 1, jnp.zeros_like(t), pltpu.roll(t, half - 1, 0))

            z = dot(cat([e, o, nxt(e), e4, o4, nxt(e4)], 1), wd[...])
            zb[n] = z
            return add_stats(carry, z)

        return lax.fori_loop(0, GROUP, one, carry)

    m = moments(1, lax.fori_loop(0, n_grp, stage_d, zero_stats), count_b, bn_down[...])

    def ex_copy(slot, g, src, dst, dev):
        part = pl.ds(g * GROUP, GROUP)
        return remote(src.at[1 - slot, part], dst.at[slot, part], ex_send.at[slot, g], ex_recv.at[slot, g], dev)

    def ex_start(g, src, dst):
        @pl.when(has_dn)
        def _():
            ex_copy(0, g, src, dst, dn).start()

        @pl.when(has_up)
        def _():
            ex_copy(1, g, src, dst, up).start()

    def ex_wait_send(src, dst):
        @pl.loop(0, n_grp)
        def _(g):
            @pl.when(has_dn)
            def _():
                ex_copy(0, g, src, dst, dn).wait_send()

            @pl.when(has_up)
            def _():
                ex_copy(1, g, src, dst, up).wait_send()

    def get(ref, part):
        return cat([ref[0, part].reshape(rows, 128), ref[1, part].reshape(rows, 128)], 1)

    def put(ref, part, v):
        ref[0, part] = v[:, :128].reshape(GROUP, half, 128)
        ref[1, part] = v[:, 128:].reshape(GROUP, half, 128)

    lane = lax.broadcasted_iota(jnp.int32, (1, 256), 1)
    valid = ((lane < 128) & has_up) | ((lane >= 128) & has_dn)

    for j in range(blocks):
        m_prev = m
        src, dst = (hb, hh) if j == 0 else (ub, rb)

        def conv_in(g, carry):
            part = pl.ds(g * GROUP, GROUP)
            z = zb[part].reshape(rows, 256)
            if j == 0:
                h = norm(z, m_prev).astype(BF)
            else:
                h = jnp.maximum((z - m_prev[0]) * m_prev[1] + m_prev[2] + get(hb, part).astype(F32), 0.0).astype(BF)
            put(hb, part, h)
            if j == 0:
                @pl.when(g > 0)
                def _():
                    ex_start(g - 1, src, dst)
            z = dot(h, w_in[j])
            zb[part] = z.reshape(GROUP, half, 256)
            return add_stats(carry, z)

        stats = lax.fori_loop(0, n_grp, conv_in, zero_stats)
        if j == 0:
            ex_start(n_grp - 1, src, dst)
        m_in = moments(2 + 3 * j, stats, count_b, bn_in[j])

        def mid_local(g, carry):
            part = pl.ds(g * GROUP, GROUP)
            u = norm(zb[part].reshape(rows, 256), m_in).astype(BF)
            zb[part] = dot(shifts(u), w_loc[j]).reshape(GROUP, half, 256)
            return carry

        lax.fori_loop(0, n_grp, mid_local, 0)

        def mid_halo(g, carry):
            part = pl.ds(g * GROUP, GROUP)

            @pl.when(has_up)
            def _():
                ex_copy(0, g, src, dst, dn).wait_recv()

            @pl.when(has_dn)
            def _():
                ex_copy(1, g, src, dst, up).wait_recv()

            h = get(hh, part)
            if j > 0:
                z = dot(get(rb, part), w_out[j - 1])
                h = jnp.maximum((z - m_prev[0]) * m_prev[1] + m_prev[2] + h.astype(F32), 0.0).astype(BF)
                if j < blocks - 1:
                    put(hh, part, h)
            u = jnp.where(valid, norm(dot(h, w_in[j]), m_in), 0.0).astype(BF)
            z = zb[part].reshape(rows, 256) + dot(shifts(u), w_halo[j])
            zb[part] = z.reshape(GROUP, half, 256)
            return add_stats(carry, z)

        stats = lax.fori_loop(0, n_grp, mid_halo, zero_stats)
        ex_wait_send(src, dst)
        m_mid = moments(3 + 3 * j, stats, count_b, bn_mid[j])

        def conv_out(g, carry):
            part = pl.ds(g * GROUP, GROUP)
            u = norm(zb[part].reshape(rows, 256), m_mid).astype(BF)
            if j < blocks - 1:
                put(ub, part, u)

                @pl.when(g > 0)
                def _():
                    ex_start(g - 1, ub, rb)
            z = dot(u, w_out[j])
            zb[part] = z.reshape(GROUP, half, 256)
            return add_stats(carry, z)

        stats = lax.fori_loop(0, n_grp, conv_out, zero_stats)
        if j < blocks - 1:
            ex_start(n_grp - 1, ub, rb)
        m = moments(4 + 3 * j, stats, count_b, bn_out[j])

    def out_copy(g, r):
        part = pl.ds(g * GROUP, GROUP)
        return pltpu.make_async_copy(hb.at[r, part], out.at[part, r], out_sem.at[r, g])

    def finish(g, carry):
        part = pl.ds(g * GROUP, GROUP)
        z = zb[part].reshape(rows, 256)
        h = jnp.maximum((z - m[0]) * m[1] + m[2] + get(hb, part).astype(F32), 0.0).astype(BF)
        put(hb, part, h)
        for r in range(2):
            out_copy(g, r).start()
        return carry

    lax.fori_loop(0, n_grp, finish, 0)

    @pl.loop(0, n_grp)
    def _(g):
        for r in range(2):
            out_copy(g, r).wait()

        @pl.when(has_dn)
        def _():
            img_copy(0, g, dn).wait_send()

        @pl.when(has_up)
        def _():
            img_copy(1, g, up).wait_send()
            img_copy(2, g, up).wait_send()

    @pl.loop(0, 2 + 3 * blocks)
    def _(k):
        remote(msg.at[k], pslot.at[k], ar_send.at[k, 0], ar_recv.at[k, 3], me).wait_send()
        for c in range(2):
            remote(cmsg.at[k], slots.at[k, 0], ar_send.at[k, 1 + c], ar_recv.at[k, 0], me).wait_send()

        @pl.when(core == OPP_CORE)
        def _():
            for c in range(2):
                remote(cmsg.at[k], slots.at[k, 2], ar_send.at[k, 3 + c], ar_recv.at[k, 2], me).wait_send()


def solution(mesh):
    sp_n = mesh.shape["sp"]

    def forward(images, w_a, bn_a, w_down, bn_down, w_in, bn_in, w_mid, bn_mid, w_out, bn_out):
        n_img, rows_dev, width, chan = images.shape
        half = width // 2
        blocks = w_in.shape[0]
        n_bn = 2 + 3 * blocks
        n_grp = n_img // GROUP
        x = jnp.transpose(images, (0, 1, 3, 2))
        dims = (n_img, width, sp_n, blocks, n_img * rows_dev * width * sp_n, n_img * (rows_dev // 2) * half * sp_n)
        vmem = pl.BlockSpec(memory_space=pltpu.VMEM)
        anys = pl.BlockSpec(memory_space=pl.ANY)
        plane = (2, n_img, half, 128)
        return pl.pallas_call(
            functools.partial(body, dims),
            out_shape=jax.ShapeDtypeStruct((n_img, rows_dev // 2, half, 128), BF),
            in_specs=[anys] * 6 + [vmem] * 5,
            out_specs=anys,
            scratch_shapes=[
                pltpu.VMEM(w_a.shape, BF),
                pltpu.VMEM(w_down.shape, BF),
                pltpu.VMEM(w_in.shape, BF),
                pltpu.VMEM(w_mid.shape, BF),
                pltpu.VMEM(w_out.shape, BF),
                pltpu.VMEM((1152, 256), BF),
                pltpu.VMEM((768, 128), BF),
                pltpu.VMEM((1152, 256), BF),
                pltpu.VMEM((blocks, 256, 256), BF),
                pltpu.VMEM((blocks, 256, 256), BF),
                pltpu.VMEM((blocks, 768, 256), BF),
                pltpu.VMEM((blocks, 768, 256), BF),
                pltpu.VMEM((SLOTS, rows_dev, chan, width), BF),
                pltpu.VMEM((3, n_img, chan, width), BF),
                pltpu.VMEM((n_img, width, 128), BF),
                pltpu.VMEM((2, n_img, width, 128), F32),
                pltpu.VMEM((width, 128), F32),
                pltpu.VMEM((n_img, half, 256), F32),
                pltpu.VMEM(plane, BF),
                pltpu.VMEM(plane, BF),
                pltpu.VMEM(plane, BF),
                pltpu.VMEM(plane, BF),
                pltpu.VMEM((n_bn, 16, 128), F32),
                pltpu.VMEM((n_bn, 16, 128), F32),
                pltpu.VMEM((n_bn, 16, 128), F32),
                pltpu.VMEM((n_bn, 3, 16, 128), F32),
                pltpu.SemaphoreType.DMA((SLOTS,)),
                pltpu.SemaphoreType.DMA((3, n_grp)),
                pltpu.SemaphoreType.DMA((3, n_grp)),
                pltpu.SemaphoreType.DMA((2, n_grp)),
                pltpu.SemaphoreType.DMA((2, n_grp)),
                pltpu.SemaphoreType.DMA((n_bn, 5)),
                pltpu.SemaphoreType.DMA((n_bn, 4)),
                pltpu.SemaphoreType.DMA((2, n_grp)),
                pltpu.SemaphoreType.DMA((5,)),
            ],
            compiler_params=pltpu.CompilerParams(
                collective_id=0, has_side_effects=True, vmem_limit_bytes=67043328),
            name="stack",
        )(x, w_a, w_down, w_in, w_mid, w_out, bn_a, bn_down, bn_in, bn_mid, bn_out)

    act_spec = P("dp", "sp", None, None)
    return jax.shard_map(forward, mesh=mesh, in_specs=(act_spec,) + (P(),) * 10, out_specs=act_spec, check_vma=False)
```

```python
import functools

import jax
import jax.numpy as jnp
from jax import lax
from jax.experimental import pallas as pl
from jax.experimental.pallas import tpu as pltpu
from jax.sharding import PartitionSpec as P

NORM_EPS = 1e-5
BF = jnp.bfloat16
F32 = jnp.float32
GROUP = 4


def cat(parts, axis):
    return jnp.concatenate(parts, axis=axis)


def banded(taps, rows_in, rows_out, stride, first):
    zero = jnp.zeros_like(taps[0])
    rows = []
    for ri in rows_in:
        cols = []
        for ro in rows_out:
            dy = ri + first - stride * ro
            cols.append(taps[dy] if 0 <= dy < len(taps) else zero)
        rows.append(cat(cols, 1))
    return cat(rows, 0)


def pack_stage_a(w_a, w_down, wa, w4, wd):
    for dx in range(3):
        ta = [w_a[0, dy, dx] for dy in range(3)]
        zero = jnp.zeros_like(ta[0])
        wa[pl.ds(dx * 384, 384)] = banded(ta, range(6), range(4), 1, 0)
        w4[pl.ds(dx * 256, 256)] = cat([cat([t, t], 1) for t in ta + [zero]], 0)
        td = [w_down[dy, dx] for dy in range(3)]
        wd[pl.ds(dx * 256, 256)] = banded(td, range(4), range(2), 2, 0)
        none = jnp.zeros_like(td[2])
        wd[pl.ds(768 + dx * 64, 64)] = cat([none, td[2]], 1)
    wd[pl.ds(960, 64)] = jnp.zeros((64, 256), BF)


def pack_stage_b(w_in, w_mid, w_out, in2, out2, mid2):
    def diag(a, b):
        z = jnp.zeros_like(a)
        return cat([cat([a, z], 1), cat([z, b], 1)], 0)

    for j in range(w_in.shape[0]):
        in2[j] = diag(w_in[j], w_in[j])
        out2[j] = diag(w_out[j], w_out[j])
        for dx in range(3):
            tm = [w_mid[j, dy, dx] for dy in range(3)]
            mid2[j, pl.ds(dx * 256, 256)] = banded(tm, (0, 1), (0, 1), 1, 1)
            mid2[j, pl.ds(768 + dx * 256, 256)] = diag(tm[0], tm[2])


def body(
    dims, img, w_a_hbm, w_down_hbm, w_in_hbm, w_mid_hbm, w_out_hbm, bn_a, bn_down, bn_in, bn_mid, bn_out, out,
    w_a_raw, w_down_raw, w_in_raw, w_mid_raw, w_out_raw, wa, w4, wd, w_in, w_out, w_mid,
    xb, halo, za, z4, zb, hb, ub, hh, rb,
    msg, pslot, cmsg, slots,
    ld_sem, im_send, im_recv, ex_send, ex_recv, ar_send, ar_recv, out_sem, w_sem,
):
    n_img, width, sp_n, blocks, count_a, count_b = dims
    half = width // 2
    n_grp = n_img // GROUP
    rows = GROUP * half
    fold = rows // width
    me = lax.axis_index("sp")
    core = lax.rem(me, 2)
    chip = lax.div(me, 2)
    chips = sp_n // 2
    has_up = me > 0
    has_dn = me < sp_n - 1
    up = jnp.maximum(me - 1, 0)
    dn = jnp.minimum(me + 1, sp_n - 1)

    def remote(src, dst, ssem, rsem, dev):
        return pltpu.make_async_remote_copy(
            src_ref=src, dst_ref=dst, send_sem=ssem, recv_sem=rsem,
            device_id={"sp": dev}, device_id_type=pl.DeviceIdType.MESH)

    w_copies = [
        pltpu.make_async_copy(src, dst, w_sem.at[i]) for i, (src, dst) in enumerate((
            (w_a_hbm, w_a_raw), (w_down_hbm, w_down_raw), (w_in_hbm, w_in_raw), (w_mid_hbm, w_mid_raw), (w_out_hbm, w_out_raw)))]
    for copy in w_copies:
        copy.start()

    def load(g):
        slot = lax.rem(g, 2)
        return pltpu.make_async_copy(img.at[pl.ds(g * GROUP, GROUP)], xb.at[slot], ld_sem.at[slot])

    load(0).start()

    bar = pltpu.get_barrier_semaphore()
    for k in range(1, sp_n):
        pl.semaphore_signal(bar, inc=1, device_id={"sp": lax.rem(me + k, sp_n)}, device_id_type=pl.DeviceIdType.MESH)
    pl.semaphore_wait(bar, sp_n - 1)

    def img_copy(slot, g, dev):
        row = (3, 0, 1)[slot]
        part = pl.ds(g * GROUP, GROUP)
        return remote(img.at[part, row], halo.at[slot, part], im_send.at[slot, g], im_recv.at[slot, g], dev)

    @pl.loop(0, n_grp)
    def _(g):
        @pl.when(has_dn)
        def _():
            img_copy(0, g, dn).start()

        @pl.when(has_up)
        def _():
            img_copy(1, g, up).start()

    @pl.when(has_up)
    def _():
        @pl.loop(0, n_grp)
        def _(g):
            img_copy(2, g, up).start()

    @pl.when(jnp.logical_not(has_up))
    def _():
        @pl.loop(0, n_img)
        def _(n):
            halo[0, n] = jnp.zeros(halo.shape[2:], BF)
            hh[0, n] = jnp.zeros(hh.shape[2:], BF)
            rb[0, n] = jnp.zeros(rb.shape[2:], BF)

    @pl.when(jnp.logical_not(has_dn))
    def _():
        @pl.loop(0, n_img)
        def _(n):
            halo[1, n] = jnp.zeros(halo.shape[2:], BF)
            halo[2, n] = jnp.zeros(halo.shape[2:], BF)
            hh[1, n] = jnp.zeros(hh.shape[2:], BF)
            rb[1, n] = jnp.zeros(rb.shape[2:], BF)

    def dot(a, b):
        return jnp.dot(a, b, preferred_element_type=F32)

    def add_stats(carry, z):
        s, q = carry
        zz = z.reshape(z.shape[0] // 8, 8, z.shape[1])
        return s + jnp.sum(zz, axis=0), q + jnp.sum(zz * zz, axis=0)

    zero_stats = (jnp.zeros((8, 256), F32), jnp.zeros((8, 256), F32))

    def norm(z, m):
        return jnp.maximum((z - m[0]) * m[1] + m[2], 0.0)

    def moments(k, stats, count, p, fold64=False, meanwhile=None):
        s, q = (t[:, :128] + t[:, 128:] for t in stats)
        if fold64:
            s, q = s + pltpu.roll(s, 64, 1), q + pltpu.roll(q, 64, 1)
        own = cat([s, q], 0)
        msg[k] = own
        first = remote(msg.at[k], pslot.at[k], ar_send.at[k, 0], ar_recv.at[k, 3], me + 1 - 2 * core)
        first.start()
        first.wait_recv()
        mine = own + pslot[k]
        cmsg[k] = mine
        near = lax.rem(chip + 1 + core * (chips - 2), chips)
        far = lax.rem(chip + 2, chips)
        for c in range(2):
            remote(cmsg.at[k], slots.at[k, core], ar_send.at[k, 1 + c], ar_recv.at[k, core], near * 2 + c).start()

        @pl.when(core == lax.rem(chip, 2))
        def _():
            for c in range(2):
                remote(cmsg.at[k], slots.at[k, 2], ar_send.at[k, 3 + c], ar_recv.at[k, 2], far * 2 + c).start()

        if meanwhile is not None:
            meanwhile()
        for c in range(3):
            remote(cmsg.at[k], slots.at[k, c], ar_send.at[k, 1], ar_recv.at[k, c], me).wait_recv()
        tot = (mine + slots[k, 2]) + (slots[k, 0] + slots[k, 1])
        inv = 1.0 / count
        mean = jnp.sum(tot[:8], axis=0, keepdims=True) * inv
        var = jnp.sum(tot[8:], axis=0, keepdims=True) * inv - mean * mean
        scale = p[0:1] * lax.rsqrt(var + NORM_EPS)
        return tuple(cat([t, t], 1) for t in (mean, scale, p[1:2]))

    def shifts(u, line):
        row = lax.rem(lax.broadcasted_iota(jnp.int32, (u.shape[0], 1), 0), line)
        zero = jnp.zeros_like(u)
        prev = jnp.where(row == 0, zero, pltpu.roll(u, 1, 0))
        nxt = jnp.where(row == line - 1, zero, pltpu.roll(u, u.shape[0] - 1, 0))
        return cat([prev, u, nxt], 1)

    for copy in w_copies:
        copy.wait()
    pack_stage_a(w_a_raw, w_down_raw, wa, w4, wd)
    pack_stage_b(w_in_raw, w_mid_raw, w_out_raw, w_in, w_out, w_mid)

    def stage_a(g, carry):
        @pl.when(g + 1 < n_grp)
        def _():
            load(g + 1).start()

        @pl.when(has_up)
        def _():
            img_copy(0, g, dn).wait_recv()

        @pl.when(has_dn)
        def _():
            img_copy(1, g, up).wait_recv()

        load(g).wait()
        for i in range(GROUP):
            n = g * GROUP + i
            x = xb.at[lax.rem(g, 2), i]
            t0 = cat([halo[0, n], x[0]], 0).T
            t1 = cat([x[1], x[2]], 0).T
            t2 = cat([x[3], halo[1, n]], 0).T
            hb[0, n] = t2[:half]
            hb[1, n] = t2[half:]
            z = dot(shifts(cat([t0, t1, t2], 1), width), wa[...])
            za[0, n] = z[:, :128]
            za[1, n] = z[:, 128:]
            carry = add_stats(carry, z)
        return carry

    m = moments(0, lax.fori_loop(0, n_grp, stage_a, zero_stats), count_a, cat([bn_a[0], bn_a[0]], 1), True)
    m_half = tuple(t[:, :128] for t in m)

    low = lax.broadcasted_iota(jnp.int32, (1, 128), 1) < 64

    def stage_d(g, carry):
        @pl.when(has_dn)
        def _():
            img_copy(2, g, up).wait_recv()

        for i in range(GROUP):
            n = g * GROUP + i
            t2 = cat([hb[0, n], hb[1, n]], 0)
            t3 = cat([halo[2, n], halo[2, n]], 0).T
            z4[i] = dot(shifts(cat([t2, t3], 1), width), w4[...])
        for i in range(GROUP):
            n = g * GROUP + i
            ev, od = pl.ds(0, half, stride=2), pl.ds(1, half, stride=2)
            e = norm(cat([za[0, n, ev, :], za[1, n, ev, :]], 1), m).astype(BF)
            o = norm(cat([za[0, n, od, :], za[1, n, od, :]], 1), m).astype(BF)
            b4 = jnp.where(has_dn, norm(jnp.where(low, z4[i, ev, :], z4[i, od, :]), m_half), 0.0).astype(BF)
            row = lax.broadcasted_iota(jnp.int32, (half, 1), 0)

            def nxt(t):
                return jnp.where(row == half - 1, jnp.zeros_like(t), pltpu.roll(t, half - 1, 0))

            z = dot(cat([e, o, nxt(e), b4, nxt(b4)], 1), wd[...])
            zb[n] = z
            carry = add_stats(carry, z)
        return carry

    m = moments(1, lax.fori_loop(0, n_grp, stage_d, zero_stats), count_b, bn_down[...])

    def ex_copy(slot, g, src, dst, dev):
        part = pl.ds(g * GROUP, GROUP)
        return remote(src.at[1 - slot, part], dst.at[slot, part], ex_send.at[slot, g], ex_recv.at[slot, g], dev)

    def ex_start(g, src, dst):
        @pl.when(has_dn)
        def _():
            ex_copy(0, g, src, dst, dn).start()

        @pl.when(has_up)
        def _():
            ex_copy(1, g, src, dst, up).start()

    def ex_wait_send(src, dst):
        @pl.loop(0, n_grp)
        def _(g):
            @pl.when(has_dn)
            def _():
                ex_copy(0, g, src, dst, dn).wait_send()

            @pl.when(has_up)
            def _():
                ex_copy(1, g, src, dst, up).wait_send()

    def get(ref, part):
        return cat([ref[0, part].reshape(rows, 128), ref[1, part].reshape(rows, 128)], 1)

    def put(ref, part, v):
        ref[0, part] = v[:, :128].reshape(GROUP, half, 128)
        ref[1, part] = v[:, 128:].reshape(GROUP, half, 128)

    lane = lax.broadcasted_iota(jnp.int32, (1, 256), 1)
    valid = ((lane < 128) & has_up) | ((lane >= 128) & has_dn)

    for j in range(blocks):
        m_prev = m
        src, dst = (hb, hh) if j == 0 else (ub, rb)

        def conv_in(g, carry):
            part = pl.ds(g * GROUP, GROUP)
            z = zb[part].reshape(rows, 256)
            if j == 0:
                h = norm(z, m_prev).astype(BF)
            else:
                h = jnp.maximum((z - m_prev[0]) * m_prev[1] + m_prev[2] + get(hb, part).astype(F32), 0.0).astype(BF)
            put(hb, part, h)
            if j == 0:
                @pl.when(g > 0)
                def _():
                    ex_start(g - 1, src, dst)
            z = dot(h, w_in[j])
            zb[part] = z.reshape(GROUP, half, 256)
            return add_stats(carry, z)

        stats = lax.fori_loop(0, n_grp, conv_in, zero_stats)
        if j == 0:
            ex_start(n_grp - 1, src, dst)
        def prep(g, slot):
            part = pl.ds(g * GROUP, GROUP)

            @pl.when(has_up)
            def _():
                ex_copy(0, g, src, dst, dn).wait_recv()

            @pl.when(has_dn)
            def _():
                ex_copy(1, g, src, dst, up).wait_recv()

            h = get(hh, part)
            if j > 0:
                z = dot(get(rb, part), w_out[j - 1])
                h = jnp.maximum((z - m_prev[0]) * m_prev[1] + m_prev[2] + h.astype(F32), 0.0).astype(BF)
                if j < blocks - 1:
                    put(hh, part, h)
            z = dot(h, w_in[j])
            for c in range(2):
                za[c, pl.ds(slot * fold, fold)] = z[:, c * 128:(c + 1) * 128].reshape(fold, width, 128)

        def main(g, slot, carry):
            part = pl.ds(g * GROUP, GROUP)
            zh = cat([za[c, pl.ds(slot * fold, fold)].reshape(rows, 128) for c in range(2)], 1)
            u = norm(zb[part].reshape(rows, 256), m_in).astype(BF)
            v = jnp.where(valid, norm(zh, m_in), 0.0).astype(BF)
            z = dot(cat([shifts(u, half), shifts(v, half)], 1), w_mid[j])
            zb[part] = z.reshape(GROUP, half, 256)
            return add_stats(carry, z)

        m_in = moments(2 + 3 * j, stats, count_b, bn_in[j], meanwhile=lambda: prep(0, 0))

        def conv_mid(i, carry):
            prep(2 * i + 1, 1)
            carry = main(2 * i, 0, carry)
            prep(2 * i + 2, 0)
            return main(2 * i + 1, 1, carry)

        stats = lax.fori_loop(0, n_grp // 2 - 1, conv_mid, zero_stats)
        prep(n_grp - 1, 1)
        stats = main(n_grp - 1, 1, main(n_grp - 2, 0, stats))
        ex_wait_send(src, dst)
        m_mid = moments(3 + 3 * j, stats, count_b, bn_mid[j])

        def conv_out(g, carry):
            part = pl.ds(g * GROUP, GROUP)
            u = norm(zb[part].reshape(rows, 256), m_mid).astype(BF)
            if j < blocks - 1:
                put(ub, part, u)

                @pl.when(g > 0)
                def _():
                    ex_start(g - 1, ub, rb)
            z = dot(u, w_out[j])
            zb[part] = z.reshape(GROUP, half, 256)
            return add_stats(carry, z)

        stats = lax.fori_loop(0, n_grp, conv_out, zero_stats)
        if j < blocks - 1:
            ex_start(n_grp - 1, ub, rb)
        m = moments(4 + 3 * j, stats, count_b, bn_out[j])

    def out_copy(g, r):
        part = pl.ds(g * GROUP, GROUP)
        return pltpu.make_async_copy(hb.at[r, part], out.at[part, r], out_sem.at[r, g])

    def finish(g, carry):
        part = pl.ds(g * GROUP, GROUP)
        z = zb[part].reshape(rows, 256)
        h = jnp.maximum((z - m[0]) * m[1] + m[2] + get(hb, part).astype(F32), 0.0).astype(BF)
        put(hb, part, h)
        for r in range(2):
            out_copy(g, r).start()
        return carry

    lax.fori_loop(0, n_grp, finish, 0)

    @pl.loop(0, n_grp)
    def _(g):
        for r in range(2):
            out_copy(g, r).wait()

        @pl.when(has_dn)
        def _():
            img_copy(0, g, dn).wait_send()

        @pl.when(has_up)
        def _():
            img_copy(1, g, up).wait_send()
            img_copy(2, g, up).wait_send()

    @pl.loop(0, 2 + 3 * blocks)
    def _(k):
        remote(msg.at[k], pslot.at[k], ar_send.at[k, 0], ar_recv.at[k, 3], me).wait_send()
        for c in range(2):
            remote(cmsg.at[k], slots.at[k, 0], ar_send.at[k, 1 + c], ar_recv.at[k, 0], me).wait_send()

        @pl.when(core == lax.rem(chip, 2))
        def _():
            for c in range(2):
                remote(cmsg.at[k], slots.at[k, 2], ar_send.at[k, 3 + c], ar_recv.at[k, 2], me).wait_send()


def solution(mesh):
    sp_n = mesh.shape["sp"]

    def forward(images, w_a, bn_a, w_down, bn_down, w_in, bn_in, w_mid, bn_mid, w_out, bn_out):
        n_img, rows_dev, width, chan = images.shape
        half = width // 2
        blocks = w_in.shape[0]
        n_bn = 2 + 3 * blocks
        n_grp = n_img // GROUP
        x = jnp.transpose(images, (0, 1, 3, 2))
        dims = (n_img, width, sp_n, blocks, n_img * rows_dev * width * sp_n, n_img * (rows_dev // 2) * half * sp_n)
        vmem = pl.BlockSpec(memory_space=pltpu.VMEM)
        anys = pl.BlockSpec(memory_space=pl.ANY)
        plane = (2, n_img, half, 128)
        return pl.pallas_call(
            functools.partial(body, dims),
            out_shape=jax.ShapeDtypeStruct((n_img, rows_dev // 2, half, 128), BF),
            in_specs=[anys] * 6 + [vmem] * 5,
            out_specs=anys,
            scratch_shapes=[
                pltpu.VMEM(w_a.shape, BF),
                pltpu.VMEM(w_down.shape, BF),
                pltpu.VMEM(w_in.shape, BF),
                pltpu.VMEM(w_mid.shape, BF),
                pltpu.VMEM(w_out.shape, BF),
                pltpu.VMEM((1152, 256), BF),
                pltpu.VMEM((768, 128), BF),
                pltpu.VMEM((1024, 256), BF),
                pltpu.VMEM((blocks, 256, 256), BF),
                pltpu.VMEM((blocks, 256, 256), BF),
                pltpu.VMEM((blocks, 1536, 256), BF),
                pltpu.VMEM((2, GROUP, rows_dev, chan, width), BF),
                pltpu.VMEM((3, n_img, chan, width), BF),
                pltpu.VMEM((2, n_img, width, 128), F32),
                pltpu.VMEM((GROUP, width, 128), F32),
                pltpu.VMEM((n_img, half, 256), F32),
                pltpu.VMEM(plane, BF),
                pltpu.VMEM(plane, BF),
                pltpu.VMEM(plane, BF),
                pltpu.VMEM(plane, BF),
                pltpu.VMEM((n_bn, 16, 128), F32),
                pltpu.VMEM((n_bn, 16, 128), F32),
                pltpu.VMEM((n_bn, 16, 128), F32),
                pltpu.VMEM((n_bn, 3, 16, 128), F32),
                pltpu.SemaphoreType.DMA((2,)),
                pltpu.SemaphoreType.DMA((3, n_grp)),
                pltpu.SemaphoreType.DMA((3, n_grp)),
                pltpu.SemaphoreType.DMA((2, n_grp)),
                pltpu.SemaphoreType.DMA((2, n_grp)),
                pltpu.SemaphoreType.DMA((n_bn, 5)),
                pltpu.SemaphoreType.DMA((n_bn, 4)),
                pltpu.SemaphoreType.DMA((2, n_grp)),
                pltpu.SemaphoreType.DMA((5,)),
            ],
            compiler_params=pltpu.CompilerParams(
                collective_id=0, has_side_effects=True, vmem_limit_bytes=67043328),
            name="stack",
        )(x, w_a, w_down, w_in, w_mid, w_out, bn_a, bn_down, bn_in, bn_mid, bn_out)

    act_spec = P("dp", "sp", None, None)
    return jax.shard_map(forward, mesh=mesh, in_specs=(act_spec,) + (P(),) * 10, out_specs=act_spec, check_vma=False)
```

```python
import functools

import jax
import jax.numpy as jnp
from jax import lax
from jax.experimental import pallas as pl
from jax.experimental.pallas import tpu as pltpu
from jax.sharding import PartitionSpec as P

NORM_EPS = 1e-5
BF = jnp.bfloat16
F32 = jnp.float32
GROUP = 4
BATCH = 8


def cat(parts, axis):
    return jnp.concatenate(parts, axis=axis)


def banded(taps, rows_in, rows_out, stride, first):
    zero = jnp.zeros_like(taps[0])
    rows = []
    for ri in rows_in:
        cols = []
        for ro in rows_out:
            dy = ri + first - stride * ro
            cols.append(taps[dy] if 0 <= dy < len(taps) else zero)
        rows.append(cat(cols, 1))
    return cat(rows, 0)


def pack_stage_a(w_a, w_down, wa, w4, wd):
    for dx in range(3):
        ta = [w_a[0, dy, dx] for dy in range(3)]
        zero = jnp.zeros_like(ta[0])
        wa[pl.ds(dx * 384, 384)] = banded(ta, range(6), range(4), 1, 0)
        w4[pl.ds(dx * 256, 256)] = cat([cat([t, t], 1) for t in ta + [zero]], 0)
        td = [w_down[dy, dx] for dy in range(3)]
        wd[pl.ds(dx * 256, 256)] = banded(td, range(4), range(2), 2, 0)
        none = jnp.zeros_like(td[2])
        wd[pl.ds(768 + dx * 64, 64)] = cat([none, td[2]], 1)
    wd[pl.ds(960, 64)] = jnp.zeros((64, 256), BF)


def pack_stage_b(w_in, w_mid, w_out, in2, out2, mid2):
    def diag(a, b):
        z = jnp.zeros_like(a)
        return cat([cat([a, z], 1), cat([z, b], 1)], 0)

    for j in range(w_in.shape[0]):
        in2[j] = diag(w_in[j], w_in[j])
        out2[j] = diag(w_out[j], w_out[j])
        for dx in range(3):
            tm = [w_mid[j, dy, dx] for dy in range(3)]
            mid2[j, pl.ds(dx * 256, 256)] = banded(tm, (0, 1), (0, 1), 1, 1)
            mid2[j, pl.ds(768 + dx * 256, 256)] = diag(tm[0], tm[2])


def body(
    dims, img, w_a_hbm, w_down_hbm, w_in_hbm, w_mid_hbm, w_out_hbm, bn_a, bn_down, bn_in, bn_mid, bn_out, hb,
    w_a_raw, w_down_raw, w_in_raw, w_mid_raw, w_out_raw, wa, w4, wd, w_in, w_out, w_mid,
    xb, halo, za, z4, zb, ub, hh, rb,
    msg, pslot, cmsg, slots,
    ld_sem, im_send, im_recv, ex_send, ex_recv, ar_send, ar_recv, w_sem,
):
    n_img, width, sp_n, blocks, count_a, count_b = dims
    half = width // 2
    n_grp = n_img // GROUP
    rows = GROUP * half
    n_bat = n_img // BATCH
    rows_b = BATCH * half
    chunks = BATCH // GROUP
    me = lax.axis_index("sp")
    core = lax.rem(me, 2)
    chip = lax.div(me, 2)
    chips = sp_n // 2
    has_up = me > 0
    has_dn = me < sp_n - 1
    up = jnp.maximum(me - 1, 0)
    dn = jnp.minimum(me + 1, sp_n - 1)

    def remote(src, dst, ssem, rsem, dev):
        return pltpu.make_async_remote_copy(
            src_ref=src, dst_ref=dst, send_sem=ssem, recv_sem=rsem,
            device_id={"sp": dev}, device_id_type=pl.DeviceIdType.MESH)

    w_copies = [
        pltpu.make_async_copy(src, dst, w_sem.at[i]) for i, (src, dst) in enumerate((
            (w_a_hbm, w_a_raw), (w_down_hbm, w_down_raw), (w_in_hbm, w_in_raw), (w_mid_hbm, w_mid_raw), (w_out_hbm, w_out_raw)))]
    for copy in w_copies:
        copy.start()

    def load(g):
        slot = lax.rem(g, 2)
        return pltpu.make_async_copy(img.at[pl.ds(g * GROUP, GROUP)], xb.at[slot], ld_sem.at[slot])

    load(0).start()

    bar = pltpu.get_barrier_semaphore()
    for k in range(1, sp_n):
        pl.semaphore_signal(bar, inc=1, device_id={"sp": lax.rem(me + k, sp_n)}, device_id_type=pl.DeviceIdType.MESH)
    pl.semaphore_wait(bar, sp_n - 1)

    def img_copy(slot, g, dev):
        row = (3, 0, 1)[slot]
        part = pl.ds(g * GROUP, GROUP)
        return remote(img.at[part, row], halo.at[slot, part], im_send.at[slot, g], im_recv.at[slot, g], dev)

    @pl.loop(0, n_grp)
    def _(g):
        @pl.when(has_dn)
        def _():
            img_copy(0, g, dn).start()

        @pl.when(has_up)
        def _():
            img_copy(1, g, up).start()

    @pl.when(has_up)
    def _():
        @pl.loop(0, n_grp)
        def _(g):
            img_copy(2, g, up).start()

    @pl.when(jnp.logical_not(has_up))
    def _():
        @pl.loop(0, n_img)
        def _(n):
            halo[0, n] = jnp.zeros(halo.shape[2:], BF)
            hh[0, n] = jnp.zeros(hh.shape[2:], BF)
            rb[0, n] = jnp.zeros(rb.shape[2:], BF)

    @pl.when(jnp.logical_not(has_dn))
    def _():
        @pl.loop(0, n_img)
        def _(n):
            halo[1, n] = jnp.zeros(halo.shape[2:], BF)
            halo[2, n] = jnp.zeros(halo.shape[2:], BF)
            hh[1, n] = jnp.zeros(hh.shape[2:], BF)
            rb[1, n] = jnp.zeros(rb.shape[2:], BF)

    def dot(a, b):
        return jnp.dot(a, b, preferred_element_type=F32)

    def add_stats(carry, z):
        s, q = carry
        zz = z.reshape(z.shape[0] // 8, 8, z.shape[1])
        return s + jnp.sum(zz, axis=0), q + jnp.sum(zz * zz, axis=0)

    zero_stats = (jnp.zeros((8, 256), F32), jnp.zeros((8, 256), F32))

    def norm(z, m):
        return jnp.maximum((z - m[0]) * m[1] + m[2], 0.0)

    def moments(k, stats, count, p, fold64=False, meanwhile=None):
        s, q = (t[:, :128] + t[:, 128:] for t in stats)
        if fold64:
            s, q = s + pltpu.roll(s, 64, 1), q + pltpu.roll(q, 64, 1)
        own = cat([s, q], 0)
        msg[k] = own
        first = remote(msg.at[k], pslot.at[k], ar_send.at[k, 0], ar_recv.at[k, 3], me + 1 - 2 * core)
        first.start()
        first.wait_recv()
        mine = own + pslot[k]
        cmsg[k] = mine
        near = lax.rem(chip + 1 + core * (chips - 2), chips)
        far = lax.rem(chip + 2, chips)
        for c in range(2):
            remote(cmsg.at[k], slots.at[k, core], ar_send.at[k, 1 + c], ar_recv.at[k, core], near * 2 + c).start()

        @pl.when(core == lax.rem(chip, 2))
        def _():
            for c in range(2):
                remote(cmsg.at[k], slots.at[k, 2], ar_send.at[k, 3 + c], ar_recv.at[k, 2], far * 2 + c).start()

        if meanwhile is not None:
            meanwhile()
        for c in range(3):
            remote(cmsg.at[k], slots.at[k, c], ar_send.at[k, 1], ar_recv.at[k, c], me).wait_recv()
        tot = (mine + slots[k, 2]) + (slots[k, 0] + slots[k, 1])
        inv = 1.0 / count
        mean = jnp.sum(tot[:8], axis=0, keepdims=True) * inv
        var = jnp.sum(tot[8:], axis=0, keepdims=True) * inv - mean * mean
        scale = p[0:1] * lax.rsqrt(var + NORM_EPS)
        return tuple(cat([t, t], 1) for t in (mean, scale, p[1:2]))

    def shifts(u, line):
        row = lax.rem(lax.broadcasted_iota(jnp.int32, (u.shape[0], 1), 0), line)
        zero = jnp.zeros_like(u)
        prev = jnp.where(row == 0, zero, pltpu.roll(u, 1, 0))
        nxt = jnp.where(row == line - 1, zero, pltpu.roll(u, u.shape[0] - 1, 0))
        return cat([prev, u, nxt], 1)

    for copy in w_copies:
        copy.wait()
    pack_stage_a(w_a_raw, w_down_raw, wa, w4, wd)
    pack_stage_b(w_in_raw, w_mid_raw, w_out_raw, w_in, w_out, w_mid)

    def stage_a(g, carry):
        @pl.when(g + 1 < n_grp)
        def _():
            load(g + 1).start()

        @pl.when(has_up)
        def _():
            img_copy(0, g, dn).wait_recv()

        @pl.when(has_dn)
        def _():
            img_copy(1, g, up).wait_recv()

        load(g).wait()
        for i in range(GROUP):
            n = g * GROUP + i
            x = xb.at[lax.rem(g, 2), i]
            t0 = cat([halo[0, n], x[0]], 0).T
            t1 = cat([x[1], x[2]], 0).T
            t2 = cat([x[3], halo[1, n]], 0).T
            hb[0, n] = t2[:half]
            hb[1, n] = t2[half:]
            z = dot(shifts(cat([t0, t1, t2], 1), width), wa[...])
            za[0, n] = z[:, :128]
            za[1, n] = z[:, 128:]
            carry = add_stats(carry, z)
        return carry

    m = moments(0, lax.fori_loop(0, n_grp, stage_a, zero_stats), count_a, cat([bn_a[0], bn_a[0]], 1), True)
    m_half = tuple(t[:, :128] for t in m)

    low = lax.broadcasted_iota(jnp.int32, (1, 128), 1) < 64

    def stage_d(g, carry):
        @pl.when(has_dn)
        def _():
            img_copy(2, g, up).wait_recv()

        for i in range(GROUP):
            n = g * GROUP + i
            t2 = cat([hb[0, n], hb[1, n]], 0)
            t3 = cat([halo[2, n], halo[2, n]], 0).T
            z4[i] = dot(shifts(cat([t2, t3], 1), width), w4[...])
        for i in range(GROUP):
            n = g * GROUP + i
            ev, od = pl.ds(0, half, stride=2), pl.ds(1, half, stride=2)
            e = norm(cat([za[0, n, ev, :], za[1, n, ev, :]], 1), m).astype(BF)
            o = norm(cat([za[0, n, od, :], za[1, n, od, :]], 1), m).astype(BF)
            b4 = jnp.where(has_dn, norm(jnp.where(low, z4[i, ev, :], z4[i, od, :]), m_half), 0.0).astype(BF)
            row = lax.broadcasted_iota(jnp.int32, (half, 1), 0)

            def nxt(t):
                return jnp.where(row == half - 1, jnp.zeros_like(t), pltpu.roll(t, half - 1, 0))

            z = dot(cat([e, o, nxt(e), b4, nxt(b4)], 1), wd[...])
            zb[n] = z
            carry = add_stats(carry, z)
        return carry

    m = moments(1, lax.fori_loop(0, n_grp, stage_d, zero_stats), count_b, bn_down[...])

    def ex_copy(slot, g, src, dst, dev):
        part = pl.ds(g * GROUP, GROUP)
        return remote(src.at[1 - slot, part], dst.at[slot, part], ex_send.at[slot, g], ex_recv.at[slot, g], dev)

    def ex_start(g, src, dst):
        @pl.when(has_dn)
        def _():
            ex_copy(0, g, src, dst, dn).start()

        @pl.when(has_up)
        def _():
            ex_copy(1, g, src, dst, up).start()

    def ex_wait_send(src, dst):
        @pl.loop(0, n_grp)
        def _(g):
            @pl.when(has_dn)
            def _():
                ex_copy(0, g, src, dst, dn).wait_send()

            @pl.when(has_up)
            def _():
                ex_copy(1, g, src, dst, up).wait_send()

    def get(ref, part):
        return cat([ref[r, part].reshape(part.size * half, 128) for r in range(2)], 1)

    def put(ref, part, v):
        for r in range(2):
            ref[r, part] = v[:, r * 128:(r + 1) * 128].reshape(part.size, half, 128)

    def ex_batch(g, src, dst):
        for c in range(chunks):
            ex_start(g * chunks + c, src, dst)

    lane = lax.broadcasted_iota(jnp.int32, (1, 256), 1)
    valid = ((lane < 128) & has_up) | ((lane >= 128) & has_dn)

    for j in range(blocks):
        m_prev = m
        src, dst = (hb, hh) if j == 0 else (ub, rb)

        def conv_in(g, carry):
            part = pl.ds(g * BATCH, BATCH)
            z = zb[part].reshape(rows_b, 256)
            if j == 0:
                h = norm(z, m_prev).astype(BF)
            else:
                h = jnp.maximum((z - m_prev[0]) * m_prev[1] + m_prev[2] + get(hb, part).astype(F32), 0.0).astype(BF)
            put(hb, part, h)
            if j == 0:
                @pl.when(g > 0)
                def _():
                    ex_batch(g - 1, src, dst)
            z = dot(h, w_in[j])
            zb[part] = z.reshape(BATCH, half, 256)
            return add_stats(carry, z)

        stats = lax.fori_loop(0, n_bat, conv_in, zero_stats)
        if j == 0:
            ex_batch(n_bat - 1, src, dst)

        m_in = moments(2 + 3 * j, stats, count_b, bn_in[j])

        def conv_mid(g, carry):
            part = pl.ds(g * GROUP, GROUP)

            @pl.when(has_up)
            def _():
                ex_copy(0, g, src, dst, dn).wait_recv()

            @pl.when(has_dn)
            def _():
                ex_copy(1, g, src, dst, up).wait_recv()

            h = get(hh, part)
            if j > 0:
                z = dot(get(rb, part), w_out[j - 1])
                h = jnp.maximum((z - m_prev[0]) * m_prev[1] + m_prev[2] + h.astype(F32), 0.0).astype(BF)
                if j < blocks - 1:
                    put(hh, part, h)
            zh = dot(h, w_in[j])
            u = norm(zb[part].reshape(rows, 256), m_in).astype(BF)
            z = dot(shifts(u, half), w_mid[j, :768])
            v = jnp.where(valid, norm(zh, m_in), 0.0).astype(BF)
            z = z + dot(shifts(v, half), w_mid[j, 768:])
            zb[part] = z.reshape(GROUP, half, 256)
            return add_stats(carry, z)

        stats = lax.fori_loop(0, n_grp, conv_mid, zero_stats)
        ex_wait_send(src, dst)
        m_mid = moments(3 + 3 * j, stats, count_b, bn_mid[j])

        def conv_out(g, carry):
            part = pl.ds(g * BATCH, BATCH)
            u = norm(zb[part].reshape(rows_b, 256), m_mid).astype(BF)
            if j < blocks - 1:
                put(ub, part, u)

                @pl.when(g > 0)
                def _():
                    ex_batch(g - 1, ub, rb)
            z = dot(u, w_out[j])
            zb[part] = z.reshape(BATCH, half, 256)
            return add_stats(carry, z)

        stats = lax.fori_loop(0, n_bat, conv_out, zero_stats)
        if j < blocks - 1:
            ex_batch(n_bat - 1, ub, rb)
        m = moments(4 + 3 * j, stats, count_b, bn_out[j])

    def finish(g, carry):
        part = pl.ds(g * BATCH, BATCH)
        z = zb[part].reshape(rows_b, 256)
        h = jnp.maximum((z - m[0]) * m[1] + m[2] + get(hb, part).astype(F32), 0.0).astype(BF)
        put(hb, part, h)
        return carry

    lax.fori_loop(0, n_bat, finish, 0)

    @pl.loop(0, n_grp)
    def _(g):
        @pl.when(has_dn)
        def _():
            img_copy(0, g, dn).wait_send()

        @pl.when(has_up)
        def _():
            img_copy(1, g, up).wait_send()
            img_copy(2, g, up).wait_send()

    @pl.loop(0, 2 + 3 * blocks)
    def _(k):
        remote(msg.at[k], pslot.at[k], ar_send.at[k, 0], ar_recv.at[k, 3], me).wait_send()
        for c in range(2):
            remote(cmsg.at[k], slots.at[k, 0], ar_send.at[k, 1 + c], ar_recv.at[k, 0], me).wait_send()

        @pl.when(core == lax.rem(chip, 2))
        def _():
            for c in range(2):
                remote(cmsg.at[k], slots.at[k, 2], ar_send.at[k, 3 + c], ar_recv.at[k, 2], me).wait_send()


def solution(mesh):
    sp_n = mesh.shape["sp"]

    def forward(images, w_a, bn_a, w_down, bn_down, w_in, bn_in, w_mid, bn_mid, w_out, bn_out):
        n_img, rows_dev, width, chan = images.shape
        half = width // 2
        blocks = w_in.shape[0]
        n_bn = 2 + 3 * blocks
        n_grp = n_img // GROUP
        x = jnp.transpose(images, (0, 1, 3, 2))
        dims = (n_img, width, sp_n, blocks, n_img * rows_dev * width * sp_n, n_img * (rows_dev // 2) * half * sp_n)
        vmem = pl.BlockSpec(memory_space=pltpu.VMEM)
        anys = pl.BlockSpec(memory_space=pl.ANY)
        plane = (2, n_img, half, 128)
        rows_first = pl.pallas_call(
            functools.partial(body, dims),
            out_shape=pltpu.VMEM(plane, BF),
            in_specs=[anys] * 6 + [vmem] * 5,
            out_specs=vmem,
            scratch_shapes=[
                pltpu.VMEM(w_a.shape, BF),
                pltpu.VMEM(w_down.shape, BF),
                pltpu.VMEM(w_in.shape, BF),
                pltpu.VMEM(w_mid.shape, BF),
                pltpu.VMEM(w_out.shape, BF),
                pltpu.VMEM((1152, 256), BF),
                pltpu.VMEM((768, 128), BF),
                pltpu.VMEM((1024, 256), BF),
                pltpu.VMEM((blocks, 256, 256), BF),
                pltpu.VMEM((blocks, 256, 256), BF),
                pltpu.VMEM((blocks, 1536, 256), BF),
                pltpu.VMEM((2, GROUP, rows_dev, chan, width), BF),
                pltpu.VMEM((3, n_img, chan, width), BF),
                pltpu.VMEM((2, n_img, width, 128), F32),
                pltpu.VMEM((GROUP, width, 128), F32),
                pltpu.VMEM((n_img, half, 256), F32),
                pltpu.VMEM(plane, BF),
                pltpu.VMEM(plane, BF),
                pltpu.VMEM(plane, BF),
                pltpu.VMEM((n_bn, 16, 128), F32),
                pltpu.VMEM((n_bn, 16, 128), F32),
                pltpu.VMEM((n_bn, 16, 128), F32),
                pltpu.VMEM((n_bn, 3, 16, 128), F32),
                pltpu.SemaphoreType.DMA((2,)),
                pltpu.SemaphoreType.DMA((3, n_grp)),
                pltpu.SemaphoreType.DMA((3, n_grp)),
                pltpu.SemaphoreType.DMA((2, n_grp)),
                pltpu.SemaphoreType.DMA((2, n_grp)),
                pltpu.SemaphoreType.DMA((n_bn, 5)),
                pltpu.SemaphoreType.DMA((n_bn, 4)),
                pltpu.SemaphoreType.DMA((5,)),
            ],
            compiler_params=pltpu.CompilerParams(
                collective_id=0, has_side_effects=True, vmem_limit_bytes=67043328 - 2 * n_img * half * 128 * 2),
            name="stack",
        )(x, w_a, w_down, w_in, w_mid, w_out, bn_a, bn_down, bn_in, bn_mid, bn_out)
        return jnp.transpose(rows_first, (1, 0, 2, 3))

    act_spec = P("dp", "sp", None, None)
    return jax.shard_map(forward, mesh=mesh, in_specs=(act_spec,) + (P(),) * 10, out_specs=act_spec, check_vma=False)
```

```python
import functools

import jax
import jax.numpy as jnp
from jax import lax
from jax.experimental import pallas as pl
from jax.experimental.pallas import tpu as pltpu
from jax.sharding import PartitionSpec as P

NORM_EPS = 1e-5
BF = jnp.bfloat16
F32 = jnp.float32
GROUP = 4
LATE = 1
BATCH = 8


def cat(parts, axis):
    return jnp.concatenate(parts, axis=axis)


def banded(taps, rows_in, rows_out, stride, first):
    zero = jnp.zeros_like(taps[0])
    rows = []
    for ri in rows_in:
        cols = []
        for ro in rows_out:
            dy = ri + first - stride * ro
            cols.append(taps[dy] if 0 <= dy < len(taps) else zero)
        rows.append(cat(cols, 1))
    return cat(rows, 0)


def pack_stage_a(w_a, w_down, wa, w4, wd):
    for dx in range(3):
        ta = [w_a[0, dy, dx] for dy in range(3)]
        zero = jnp.zeros_like(ta[0])
        wa[pl.ds(dx * 384, 384)] = banded(ta, range(6), range(4), 1, 0)
        w4[pl.ds(dx * 256, 256)] = cat([cat([t, t], 1) for t in ta + [zero]], 0)
        td = [w_down[dy, dx] for dy in range(3)]
        wd[pl.ds(dx * 256, 256)] = banded(td, range(4), range(2), 2, 0)
        none = jnp.zeros_like(td[2])
        wd[pl.ds(768 + dx * 64, 64)] = cat([none, td[2]], 1)
    wd[pl.ds(960, 64)] = jnp.zeros((64, 256), BF)


def pack_stage_b(w_in, w_mid, w_out, in2, out2, mid2):
    def diag(a, b):
        z = jnp.zeros_like(a)
        return cat([cat([a, z], 1), cat([z, b], 1)], 0)

    for j in range(w_in.shape[0]):
        in2[j] = diag(w_in[j], w_in[j])
        out2[j] = diag(w_out[j], w_out[j])
        for dx in range(3):
            tm = [w_mid[j, dy, dx] for dy in range(3)]
            mid2[j, pl.ds(dx * 256, 256)] = banded(tm, (0, 1), (0, 1), 1, 1)
            mid2[j, pl.ds(768 + dx * 256, 256)] = diag(tm[0], tm[2])


def body(
    dims, img, w_a_hbm, w_down_hbm, w_in_hbm, w_mid_hbm, w_out_hbm, bn_a, bn_down, bn_in, bn_mid, bn_out, hb,
    w_a_raw, w_down_raw, w_in_raw, w_mid_raw, w_out_raw, wa, w4, wd, w_in, w_out, w_mid,
    xb, halo, za, z4, zb, ub, hh, rb,
    msg, pslot, cmsg, slots,
    ld_sem, im_send, im_recv, ex_send, ex_recv, ar_send, ar_recv, w_sem, all8, d_send, d_recv,
):
    n_img, width, sp_n, blocks, count_a, count_b = dims
    half = width // 2
    n_grp = n_img // GROUP
    rows = GROUP * half
    fold = rows // width
    n_bat = n_img // BATCH
    rows_b = BATCH * half
    chunks = BATCH // GROUP
    me = lax.axis_index("sp")
    core = lax.rem(me, 2)
    chip = lax.div(me, 2)
    chips = sp_n // 2
    has_up = me > 0
    has_dn = me < sp_n - 1
    up = jnp.maximum(me - 1, 0)
    dn = jnp.minimum(me + 1, sp_n - 1)

    def remote(src, dst, ssem, rsem, dev):
        return pltpu.make_async_remote_copy(
            src_ref=src, dst_ref=dst, send_sem=ssem, recv_sem=rsem,
            device_id={"sp": dev}, device_id_type=pl.DeviceIdType.MESH)

    w_copies = [
        pltpu.make_async_copy(src, dst, w_sem.at[i]) for i, (src, dst) in enumerate((
            (w_a_hbm, w_a_raw), (w_down_hbm, w_down_raw), (w_in_hbm, w_in_raw), (w_mid_hbm, w_mid_raw), (w_out_hbm, w_out_raw)))]
    for copy in w_copies:
        copy.start()

    def load(g):
        slot = lax.rem(g, 2)
        return pltpu.make_async_copy(img.at[pl.ds(g * GROUP, GROUP)], xb.at[slot], ld_sem.at[slot])

    load(0).start()

    direct_ks = [1] + [3 + 3 * j for j in range(blocks)] + [1 + 3 * blocks]

    bar = pltpu.get_barrier_semaphore()
    for k in range(1, sp_n):
        pl.semaphore_signal(bar, inc=1, device_id={"sp": lax.rem(me + k, sp_n)}, device_id_type=pl.DeviceIdType.MESH)
    pl.semaphore_wait(bar, sp_n - 1)

    def img_copy(slot, g, dev):
        row = (3, 0, 1)[slot]
        part = pl.ds(g * GROUP, GROUP)
        return remote(img.at[part, row], halo.at[slot, part], im_send.at[slot, g], im_recv.at[slot, g], dev)

    @pl.loop(0, n_grp)
    def _(g):
        @pl.when(has_dn)
        def _():
            img_copy(0, g, dn).start()

        @pl.when(has_up)
        def _():
            img_copy(1, g, up).start()

    @pl.when(has_up)
    def _():
        @pl.loop(0, n_grp)
        def _(g):
            img_copy(2, g, up).start()

    @pl.when(jnp.logical_not(has_up))
    def _():
        @pl.loop(0, n_img)
        def _(n):
            halo[0, n] = jnp.zeros(halo.shape[2:], BF)
            hh[0, n] = jnp.zeros(hh.shape[2:], BF)
            rb[0, n] = jnp.zeros(rb.shape[2:], BF)

    @pl.when(jnp.logical_not(has_dn))
    def _():
        @pl.loop(0, n_img)
        def _(n):
            halo[1, n] = jnp.zeros(halo.shape[2:], BF)
            halo[2, n] = jnp.zeros(halo.shape[2:], BF)
            hh[1, n] = jnp.zeros(hh.shape[2:], BF)
            rb[1, n] = jnp.zeros(rb.shape[2:], BF)

    def dot(a, b):
        return jnp.dot(a, b, preferred_element_type=F32)

    def add_stats(carry, z):
        s, q = carry
        zz = z.reshape(z.shape[0] // 8, 8, z.shape[1])
        return s + jnp.sum(zz, axis=0), q + jnp.sum(zz * zz, axis=0)

    zero_stats = (jnp.zeros((8, 256), F32), jnp.zeros((8, 256), F32))

    def norm(z, m):
        return jnp.maximum((z - m[0]) * m[1] + m[2], 0.0)

    def direct(d, other):
        return remote(msg.at[direct_ks[d]], all8.at[d, me], d_send.at[d, other], d_recv.at[d, me], other)

    def moments(k, stats, count, p, fold64=False, meanwhile=None):
        s, q = (t[:, :128] + t[:, 128:] for t in stats)
        if fold64:
            s, q = s + pltpu.roll(s, 64, 1), q + pltpu.roll(q, 64, 1)
        own = cat([s, q], 0)
        msg[k] = own
        if k in direct_ks:
            d = direct_ks.index(k)
            all8[d, me] = own
            for i in range(1, sp_n):
                direct(d, lax.rem(me + i, sp_n)).start()
            for i in range(1, sp_n):
                other = lax.rem(me + i, sp_n)
                remote(msg.at[k], all8.at[d, other], d_send.at[d, other], d_recv.at[d, other], other).wait_recv()
            parts = [all8[d, i] for i in range(sp_n)]
            while len(parts) > 1:
                parts = [parts[i] + parts[i + 1] for i in range(0, len(parts), 2)]
            tot = parts[0]
        else:
            first = remote(msg.at[k], pslot.at[k], ar_send.at[k, 0], ar_recv.at[k, 3], me + 1 - 2 * core)
            first.start()
            first.wait_recv()
            mine = own + pslot[k]
            cmsg[k] = mine
            near = lax.rem(chip + 1 + core * (chips - 2), chips)
            far = lax.rem(chip + 2, chips)
            for c in range(2):
                remote(cmsg.at[k], slots.at[k, core], ar_send.at[k, 1 + c], ar_recv.at[k, core], near * 2 + c).start()

            @pl.when(core == lax.rem(chip, 2))
            def _():
                for c in range(2):
                    remote(cmsg.at[k], slots.at[k, 2], ar_send.at[k, 3 + c], ar_recv.at[k, 2], far * 2 + c).start()

            if meanwhile is not None:
                meanwhile()
            for c in range(3):
                remote(cmsg.at[k], slots.at[k, c], ar_send.at[k, 1], ar_recv.at[k, c], me).wait_recv()
            tot = (mine + slots[k, 2]) + (slots[k, 0] + slots[k, 1])
        inv = 1.0 / count
        mean = jnp.sum(tot[:8], axis=0, keepdims=True) * inv
        var = jnp.sum(tot[8:], axis=0, keepdims=True) * inv - mean * mean
        scale = p[0:1] * lax.rsqrt(var + NORM_EPS)
        return tuple(cat([t, t], 1) for t in (mean, scale, p[1:2]))

    def shifts(u, line):
        row = lax.rem(lax.broadcasted_iota(jnp.int32, (u.shape[0], 1), 0), line)
        zero = jnp.zeros_like(u)
        prev = jnp.where(row == 0, zero, pltpu.roll(u, 1, 0))
        nxt = jnp.where(row == line - 1, zero, pltpu.roll(u, u.shape[0] - 1, 0))
        return cat([prev, u, nxt], 1)

    for copy in w_copies:
        copy.wait()
    pack_stage_a(w_a_raw, w_down_raw, wa, w4, wd)
    pack_stage_b(w_in_raw, w_mid_raw, w_out_raw, w_in, w_out, w_mid)

    def stage_a(g, carry):
        @pl.when(g + 1 < n_grp)
        def _():
            load(g + 1).start()

        @pl.when(has_up)
        def _():
            img_copy(0, g, dn).wait_recv()

        @pl.when(has_dn)
        def _():
            img_copy(1, g, up).wait_recv()

        load(g).wait()
        for i in range(GROUP):
            n = g * GROUP + i
            x = xb.at[lax.rem(g, 2), i]
            t0 = cat([halo[0, n], x[0]], 0).T
            t1 = cat([x[1], x[2]], 0).T
            t2 = cat([x[3], halo[1, n]], 0).T
            hb[0, n] = t2[:half]
            hb[1, n] = t2[half:]
            z = dot(shifts(cat([t0, t1, t2], 1), width), wa[...])
            za[0, n] = z[:, :128]
            za[1, n] = z[:, 128:]
            carry = add_stats(carry, z)
        return carry

    m = moments(0, lax.fori_loop(0, n_grp, stage_a, zero_stats), count_a, cat([bn_a[0], bn_a[0]], 1), True)
    m_half = tuple(t[:, :128] for t in m)

    low = lax.broadcasted_iota(jnp.int32, (1, 128), 1) < 64

    def stage_d(g, carry):
        @pl.when(has_dn)
        def _():
            img_copy(2, g, up).wait_recv()

        for i in range(GROUP):
            n = g * GROUP + i
            t2 = cat([hb[0, n], hb[1, n]], 0)
            t3 = cat([halo[2, n], halo[2, n]], 0).T
            z4[i] = dot(shifts(cat([t2, t3], 1), width), w4[...])
        for i in range(GROUP):
            n = g * GROUP + i
            ev, od = pl.ds(0, half, stride=2), pl.ds(1, half, stride=2)
            e = norm(cat([za[0, n, ev, :], za[1, n, ev, :]], 1), m).astype(BF)
            o = norm(cat([za[0, n, od, :], za[1, n, od, :]], 1), m).astype(BF)
            b4 = jnp.where(has_dn, norm(jnp.where(low, z4[i, ev, :], z4[i, od, :]), m_half), 0.0).astype(BF)
            row = lax.broadcasted_iota(jnp.int32, (half, 1), 0)

            def nxt(t):
                return jnp.where(row == half - 1, jnp.zeros_like(t), pltpu.roll(t, half - 1, 0))

            z = dot(cat([e, o, nxt(e), b4, nxt(b4)], 1), wd[...])
            zb[n] = z
            carry = add_stats(carry, z)
        return carry

    m = moments(1, lax.fori_loop(0, n_grp, stage_d, zero_stats), count_b, bn_down[...])

    def ex_copy(slot, g, src, dst, dev):
        part = pl.ds(g * GROUP, GROUP)
        return remote(src.at[1 - slot, part], dst.at[slot, part], ex_send.at[slot, g], ex_recv.at[slot, g], dev)

    def ex_start(g, src, dst):
        @pl.when(has_dn)
        def _():
            ex_copy(0, g, src, dst, dn).start()

        @pl.when(has_up)
        def _():
            ex_copy(1, g, src, dst, up).start()

    def ex_wait_send(src, dst):
        @pl.loop(0, n_grp)
        def _(g):
            @pl.when(has_dn)
            def _():
                ex_copy(0, g, src, dst, dn).wait_send()

            @pl.when(has_up)
            def _():
                ex_copy(1, g, src, dst, up).wait_send()

    def get(ref, part):
        return cat([ref[r, part].reshape(part.size * half, 128) for r in range(2)], 1)

    def put(ref, part, v):
        for r in range(2):
            ref[r, part] = v[:, r * 128:(r + 1) * 128].reshape(part.size, half, 128)

    def ex_batch(g, src, dst):
        for c in range(chunks):
            ex_start(g * chunks + c, src, dst)

    lane = lax.broadcasted_iota(jnp.int32, (1, 256), 1)
    valid = ((lane < 128) & has_up) | ((lane >= 128) & has_dn)

    for j in range(blocks):
        m_prev = m
        src, dst = (hb, hh) if j == 0 else (ub, rb)

        def conv_in(g, carry):
            part = pl.ds(g * BATCH, BATCH)
            z = zb[part].reshape(rows_b, 256)
            if j == 0:
                h = norm(z, m_prev).astype(BF)
            else:
                h = jnp.maximum((z - m_prev[0]) * m_prev[1] + m_prev[2] + get(hb, part).astype(F32), 0.0).astype(BF)
            put(hb, part, h)
            if j == 0:
                @pl.when(g > 0)
                def _():
                    ex_batch(g - 1, src, dst)
            z = dot(h, w_in[j])
            zb[part] = z.reshape(BATCH, half, 256)
            return add_stats(carry, z)

        stats = lax.fori_loop(0, n_bat, conv_in, zero_stats)
        if j == 0:
            ex_batch(n_bat - 1, src, dst)

        def halo_rows(g, many):
            part = pl.ds(g * GROUP * many, GROUP * many)
            for c in range(many):
                @pl.when(has_up)
                def _():
                    ex_copy(0, g * many + c, src, dst, dn).wait_recv()

                @pl.when(has_dn)
                def _():
                    ex_copy(1, g * many + c, src, dst, up).wait_recv()

            h = get(hh, part)
            if j > 0:
                z = dot(get(rb, part), w_out[j - 1])
                h = jnp.maximum((z - m_prev[0]) * m_prev[1] + m_prev[2] + h.astype(F32), 0.0).astype(BF)
                if j < blocks - 1:
                    put(hh, part, h)
            return dot(h, w_in[j])

        def taps(g, many, zh, carry):
            images = GROUP * many
            part = pl.ds(g * images, images)
            u = norm(zb[part].reshape(images * half, 256), m_in).astype(BF)
            z = dot(shifts(u, half), w_mid[j, :768])
            v = jnp.where(valid, norm(zh, m_in), 0.0).astype(BF)
            z = z + dot(shifts(v, half), w_mid[j, 768:])
            zb[part] = z.reshape(images, half, 256)
            return add_stats(carry, z)

        def conv_mid(g, carry, many):
            return taps(g, many, halo_rows(g, many), carry)

        def first_pair():
            @pl.loop(0, 2)
            def _(g):
                zh = halo_rows(g, 1)
                for c in range(2):
                    za[c, pl.ds(g * fold, fold)] = zh[:, c * 128:(c + 1) * 128].reshape(fold, width, 128)

        m_in = moments(2 + 3 * j, stats, count_b, bn_in[j], meanwhile=first_pair)

        def prepared(g, carry):
            zh = cat([za[c, pl.ds(g * fold, fold)].reshape(rows, 128) for c in range(2)], 1)
            return taps(g, 1, zh, carry)

        stats = lax.fori_loop(0, 2, prepared, zero_stats)

        stats = lax.fori_loop(1, n_grp // 2 - LATE, functools.partial(conv_mid, many=2), stats)
        stats = lax.fori_loop(n_grp - 2 * LATE, n_grp, functools.partial(conv_mid, many=1), stats)
        ex_wait_send(src, dst)
        m_mid = moments(3 + 3 * j, stats, count_b, bn_mid[j])

        def conv_out(g, carry):
            part = pl.ds(g * BATCH, BATCH)
            u = norm(zb[part].reshape(rows_b, 256), m_mid).astype(BF)
            if j < blocks - 1:
                put(ub, part, u)

                @pl.when(g > 0)
                def _():
                    ex_batch(g - 1, ub, rb)
            z = dot(u, w_out[j])
            zb[part] = z.reshape(BATCH, half, 256)
            return add_stats(carry, z)

        stats = lax.fori_loop(0, n_bat, conv_out, zero_stats)
        if j < blocks - 1:
            ex_batch(n_bat - 1, ub, rb)
        m = moments(4 + 3 * j, stats, count_b, bn_out[j])

    def finish(g, carry):
        part = pl.ds(g * BATCH, BATCH)
        z = zb[part].reshape(rows_b, 256)
        h = jnp.maximum((z - m[0]) * m[1] + m[2] + get(hb, part).astype(F32), 0.0).astype(BF)
        put(hb, part, h)
        return carry

    lax.fori_loop(0, n_bat, finish, 0)

    @pl.loop(0, n_grp)
    def _(g):
        @pl.when(has_dn)
        def _():
            img_copy(0, g, dn).wait_send()

        @pl.when(has_up)
        def _():
            img_copy(1, g, up).wait_send()
            img_copy(2, g, up).wait_send()

    for k in range(2 + 3 * blocks):
        if k in direct_ks:
            d = direct_ks.index(k)
            for i in range(1, sp_n):
                direct(d, lax.rem(me + i, sp_n)).wait_send()
            continue

        remote(msg.at[k], pslot.at[k], ar_send.at[k, 0], ar_recv.at[k, 3], me).wait_send()
        for c in range(2):
            remote(cmsg.at[k], slots.at[k, 0], ar_send.at[k, 1 + c], ar_recv.at[k, 0], me).wait_send()

        @pl.when(core == lax.rem(chip, 2))
        def _():
            for c in range(2):
                remote(cmsg.at[k], slots.at[k, 2], ar_send.at[k, 3 + c], ar_recv.at[k, 2], me).wait_send()


def solution(mesh):
    sp_n = mesh.shape["sp"]

    def forward(images, w_a, bn_a, w_down, bn_down, w_in, bn_in, w_mid, bn_mid, w_out, bn_out):
        n_img, rows_dev, width, chan = images.shape
        half = width // 2
        blocks = w_in.shape[0]
        n_bn = 2 + 3 * blocks
        n_grp = n_img // GROUP
        x = jnp.transpose(images, (0, 1, 3, 2))
        dims = (n_img, width, sp_n, blocks, n_img * rows_dev * width * sp_n, n_img * (rows_dev // 2) * half * sp_n)
        vmem = pl.BlockSpec(memory_space=pltpu.VMEM)
        anys = pl.BlockSpec(memory_space=pl.ANY)
        plane = (2, n_img, half, 128)
        rows_first = pl.pallas_call(
            functools.partial(body, dims),
            out_shape=pltpu.VMEM(plane, BF),
            in_specs=[anys] * 6 + [vmem] * 5,
            out_specs=vmem,
            scratch_shapes=[
                pltpu.VMEM(w_a.shape, BF),
                pltpu.VMEM(w_down.shape, BF),
                pltpu.VMEM(w_in.shape, BF),
                pltpu.VMEM(w_mid.shape, BF),
                pltpu.VMEM(w_out.shape, BF),
                pltpu.VMEM((1152, 256), BF),
                pltpu.VMEM((768, 128), BF),
                pltpu.VMEM((1024, 256), BF),
                pltpu.VMEM((blocks, 256, 256), BF),
                pltpu.VMEM((blocks, 256, 256), BF),
                pltpu.VMEM((blocks, 1536, 256), BF),
                pltpu.VMEM((2, GROUP, rows_dev, chan, width), BF),
                pltpu.VMEM((3, n_img, chan, width), BF),
                pltpu.VMEM((2, n_img, width, 128), F32),
                pltpu.VMEM((GROUP, width, 128), F32),
                pltpu.VMEM((n_img, half, 256), F32),
                pltpu.VMEM(plane, BF),
                pltpu.VMEM(plane, BF),
                pltpu.VMEM(plane, BF),
                pltpu.VMEM((n_bn, 16, 128), F32),
                pltpu.VMEM((n_bn, 16, 128), F32),
                pltpu.VMEM((n_bn, 16, 128), F32),
                pltpu.VMEM((n_bn, 3, 16, 128), F32),
                pltpu.SemaphoreType.DMA((2,)),
                pltpu.SemaphoreType.DMA((3, n_grp)),
                pltpu.SemaphoreType.DMA((3, n_grp)),
                pltpu.SemaphoreType.DMA((2, n_grp)),
                pltpu.SemaphoreType.DMA((2, n_grp)),
                pltpu.SemaphoreType.DMA((n_bn, 5)),
                pltpu.SemaphoreType.DMA((n_bn, 4)),
                pltpu.SemaphoreType.DMA((5,)),
                pltpu.VMEM((2 + blocks, sp_n, 16, 128), F32),
                pltpu.SemaphoreType.DMA((2 + blocks, sp_n)),
                pltpu.SemaphoreType.DMA((2 + blocks, sp_n)),
            ],
            compiler_params=pltpu.CompilerParams(
                collective_id=0, has_side_effects=True, vmem_limit_bytes=67043328 - 2 * n_img * half * 128 * 2),
            name="stack",
        )(x, w_a, w_down, w_in, w_mid, w_out, bn_a, bn_down, bn_in, bn_mid, bn_out)
        return jnp.transpose(rows_first, (1, 0, 2, 3))

    act_spec = P("dp", "sp", None, None)
    return jax.shard_map(forward, mesh=mesh, in_specs=(act_spec,) + (P(),) * 10, out_specs=act_spec, check_vma=False)
```

```python
import functools

import jax
import jax.numpy as jnp
from jax import lax
from jax.experimental import pallas as pl
from jax.experimental.pallas import tpu as pltpu
from jax.sharding import PartitionSpec as P

NORM_EPS = 1e-5
BF = jnp.bfloat16
F32 = jnp.float32
GROUP = 4
LATE = 1
BATCH = 8


def cat(parts, axis):
    return jnp.concatenate(parts, axis=axis)


def banded(taps, rows_in, rows_out, stride, first):
    zero = jnp.zeros_like(taps[0])
    rows = []
    for ri in rows_in:
        cols = []
        for ro in rows_out:
            dy = ri + first - stride * ro
            cols.append(taps[dy] if 0 <= dy < len(taps) else zero)
        rows.append(cat(cols, 1))
    return cat(rows, 0)


def pack_stage_a(w_a, w_down, wa, w4, wd):
    for dx in range(3):
        ta = [w_a[0, dy, dx] for dy in range(3)]
        zero = jnp.zeros_like(ta[0])
        wa[pl.ds(dx * 384, 384)] = banded(ta, range(6), range(4), 1, 0)
        w4[pl.ds(dx * 256, 256)] = cat([cat([t, t], 1) for t in ta + [zero]], 0)
        td = [w_down[dy, dx] for dy in range(3)]
        wd[pl.ds(dx * 256, 256)] = banded(td, range(4), range(2), 2, 0)
        none = jnp.zeros_like(td[2])
        wd[pl.ds(768 + dx * 64, 64)] = cat([none, td[2]], 1)
    wd[pl.ds(960, 64)] = jnp.zeros((64, 256), BF)


def pack_stage_b(w_in, w_mid, w_out, in2, out2, mid2):
    def diag(a, b):
        z = jnp.zeros_like(a)
        return cat([cat([a, z], 1), cat([z, b], 1)], 0)

    for j in range(w_in.shape[0]):
        in2[j] = diag(w_in[j], w_in[j])
        out2[j] = diag(w_out[j], w_out[j])
        for dx in range(3):
            tm = [w_mid[j, dy, dx] for dy in range(3)]
            mid2[j, pl.ds(dx * 256, 256)] = banded(tm, (0, 1), (0, 1), 1, 1)
            mid2[j, pl.ds(768 + dx * 256, 256)] = diag(tm[0], tm[2])


def body(
    dims, img, w_a_hbm, w_down_hbm, w_in_hbm, w_mid_hbm, w_out_hbm, bn_a, bn_down, bn_in, bn_mid, bn_out, hb,
    w_a_raw, w_down_raw, w_in_raw, w_mid_raw, w_out_raw, wa, w4, wd, w_in, w_out, w_mid,
    xb, halo, za, z4, zb, ub, hh, rb,
    msg, pslot, cmsg, slots,
    ld_sem, im_send, im_recv, ex_send, ex_recv, ar_send, ar_recv, w_sem, all8, d_send, d_recv,
):
    n_img, width, sp_n, blocks, count_a, count_b = dims
    half = width // 2
    n_grp = n_img // GROUP
    rows = GROUP * half
    fold = rows // width
    n_bat = n_img // BATCH
    rows_b = BATCH * half
    chunks = BATCH // GROUP
    me = lax.axis_index("sp")
    core = lax.rem(me, 2)
    chip = lax.div(me, 2)
    chips = sp_n // 2
    has_up = me > 0
    has_dn = me < sp_n - 1
    up = jnp.maximum(me - 1, 0)
    dn = jnp.minimum(me + 1, sp_n - 1)

    def remote(src, dst, ssem, rsem, dev):
        return pltpu.make_async_remote_copy(
            src_ref=src, dst_ref=dst, send_sem=ssem, recv_sem=rsem,
            device_id={"sp": dev}, device_id_type=pl.DeviceIdType.MESH)

    w_copies = [
        pltpu.make_async_copy(src, dst, w_sem.at[i]) for i, (src, dst) in enumerate((
            (w_a_hbm, w_a_raw), (w_down_hbm, w_down_raw), (w_in_hbm, w_in_raw), (w_mid_hbm, w_mid_raw), (w_out_hbm, w_out_raw)))]
    for copy in w_copies:
        copy.start()

    def load(g):
        slot = lax.rem(g, 2)
        return pltpu.make_async_copy(img.at[pl.ds(g * GROUP, GROUP)], xb.at[slot], ld_sem.at[slot])

    load(0).start()

    direct_ks = [1] + [3 + 3 * j for j in range(blocks)] + [1 + 3 * blocks]

    bar = pltpu.get_barrier_semaphore()
    for k in range(1, sp_n):
        pl.semaphore_signal(bar, inc=1, device_id={"sp": lax.rem(me + k, sp_n)}, device_id_type=pl.DeviceIdType.MESH)
    pl.semaphore_wait(bar, sp_n - 1)

    def img_copy(slot, g, dev):
        row = (3, 0, 1)[slot]
        part = pl.ds(g * GROUP, GROUP)
        return remote(img.at[part, row], halo.at[slot, part], im_send.at[slot, g], im_recv.at[slot, g], dev)

    @pl.loop(0, n_grp)
    def _(g):
        @pl.when(has_dn)
        def _():
            img_copy(0, g, dn).start()

        @pl.when(has_up)
        def _():
            img_copy(1, g, up).start()

    @pl.when(has_up)
    def _():
        @pl.loop(0, n_grp)
        def _(g):
            img_copy(2, g, up).start()

    @pl.when(jnp.logical_not(has_up))
    def _():
        @pl.loop(0, n_img)
        def _(n):
            halo[0, n] = jnp.zeros(halo.shape[2:], BF)
            hh[0, n] = jnp.zeros(hh.shape[2:], BF)
            rb[0, n] = jnp.zeros(rb.shape[2:], BF)

    @pl.when(jnp.logical_not(has_dn))
    def _():
        @pl.loop(0, n_img)
        def _(n):
            halo[1, n] = jnp.zeros(halo.shape[2:], BF)
            halo[2, n] = jnp.zeros(halo.shape[2:], BF)
            hh[1, n] = jnp.zeros(hh.shape[2:], BF)
            rb[1, n] = jnp.zeros(rb.shape[2:], BF)

    def dot(a, b):
        return jnp.dot(a, b, preferred_element_type=F32)

    def add_stats(carry, z):
        s, q = carry
        zz = z.reshape(z.shape[0] // 8, 8, z.shape[1])
        return s + jnp.sum(zz, axis=0), q + jnp.sum(zz * zz, axis=0)

    zero_stats = (jnp.zeros((8, 256), F32), jnp.zeros((8, 256), F32))

    def norm(z, m):
        return jnp.maximum((z - m[0]) * m[1] + m[2], 0.0)

    def direct(d, other):
        return remote(msg.at[direct_ks[d]], all8.at[d, me], d_send.at[d, other], d_recv.at[d, me], other)

    def moments(k, stats, count, p, fold64=False, meanwhile=None):
        s, q = (t[:, :128] + t[:, 128:] for t in stats)
        if fold64:
            s, q = s + pltpu.roll(s, 64, 1), q + pltpu.roll(q, 64, 1)
        own = cat([jnp.sum(s, axis=0, keepdims=True), jnp.sum(q, axis=0, keepdims=True), jnp.zeros((6, 128), F32)], 0)
        msg[k] = own
        if k in direct_ks:
            d = direct_ks.index(k)
            all8[d, me] = own
            for i in sorted(range(1, sp_n), key=lambda i: abs(i - chips)):
                direct(d, lax.rem(me + i, sp_n)).start()
            for i in range(1, sp_n):
                other = lax.rem(me + i, sp_n)
                remote(msg.at[k], all8.at[d, other], d_send.at[d, other], d_recv.at[d, other], other).wait_recv()
            parts = [all8[d, i] for i in range(sp_n)]
            while len(parts) > 1:
                parts = [parts[i] + parts[i + 1] for i in range(0, len(parts), 2)]
            tot = parts[0]
        else:
            first = remote(msg.at[k], pslot.at[k], ar_send.at[k, 0], ar_recv.at[k, 3], me + 1 - 2 * core)
            first.start()
            first.wait_recv()
            mine = own + pslot[k]
            cmsg[k] = mine
            near = lax.rem(chip + 1 + core * (chips - 2), chips)
            far = lax.rem(chip + 2, chips)
            @pl.when(core == lax.rem(chip, 2))
            def _():
                for c in range(2):
                    remote(cmsg.at[k], slots.at[k, 2], ar_send.at[k, 3 + c], ar_recv.at[k, 2], far * 2 + c).start()

            for c in range(2):
                remote(cmsg.at[k], slots.at[k, core], ar_send.at[k, 1 + c], ar_recv.at[k, core], near * 2 + c).start()

            if meanwhile is not None:
                meanwhile()
            for c in range(3):
                remote(cmsg.at[k], slots.at[k, c], ar_send.at[k, 1], ar_recv.at[k, c], me).wait_recv()
            tot = (mine + slots[k, 2]) + (slots[k, 0] + slots[k, 1])
        inv = 1.0 / count
        mean = tot[0:1] * inv
        var = tot[1:2] * inv - mean * mean
        scale = p[0:1] * lax.rsqrt(var + NORM_EPS)
        return tuple(cat([t, t], 1) for t in (mean, scale, p[1:2]))

    def shifts(u, line):
        row = lax.rem(lax.broadcasted_iota(jnp.int32, (u.shape[0], 1), 0), line)
        zero = jnp.zeros_like(u)
        prev = jnp.where(row == 0, zero, pltpu.roll(u, 1, 0))
        nxt = jnp.where(row == line - 1, zero, pltpu.roll(u, u.shape[0] - 1, 0))
        return cat([prev, u, nxt], 1)

    for copy in w_copies:
        copy.wait()
    pack_stage_a(w_a_raw, w_down_raw, wa, w4, wd)
    pack_stage_b(w_in_raw, w_mid_raw, w_out_raw, w_in, w_out, w_mid)

    def stage_a(g, carry):
        @pl.when(g + 1 < n_grp)
        def _():
            load(g + 1).start()

        @pl.when(has_up)
        def _():
            img_copy(0, g, dn).wait_recv()

        @pl.when(has_dn)
        def _():
            img_copy(1, g, up).wait_recv()

        load(g).wait()
        for i in range(GROUP):
            n = g * GROUP + i
            x = xb.at[lax.rem(g, 2), i]
            t0 = cat([halo[0, n], x[0]], 0).T
            t1 = cat([x[1], x[2]], 0).T
            t2 = cat([x[3], halo[1, n]], 0).T
            hb[0, n] = t2[:half]
            hb[1, n] = t2[half:]
            z = dot(shifts(cat([t0, t1, t2], 1), width), wa[...])
            za[0, n] = z[:, :128]
            za[1, n] = z[:, 128:]
            carry = add_stats(carry, z)
        return carry

    m = moments(0, lax.fori_loop(0, n_grp, stage_a, zero_stats), count_a, cat([bn_a[0], bn_a[0]], 1), True)
    m_half = tuple(t[:, :128] for t in m)

    low = lax.broadcasted_iota(jnp.int32, (1, 128), 1) < 64

    def stage_d(g, carry):
        @pl.when(has_dn)
        def _():
            img_copy(2, g, up).wait_recv()

        for i in range(GROUP):
            n = g * GROUP + i
            t2 = cat([hb[0, n], hb[1, n]], 0)
            t3 = cat([halo[2, n], halo[2, n]], 0).T
            z4[i] = dot(shifts(cat([t2, t3], 1), width), w4[...])
        for i in range(GROUP):
            n = g * GROUP + i
            ev, od = pl.ds(0, half, stride=2), pl.ds(1, half, stride=2)
            e = norm(cat([za[0, n, ev, :], za[1, n, ev, :]], 1), m).astype(BF)
            o = norm(cat([za[0, n, od, :], za[1, n, od, :]], 1), m).astype(BF)
            b4 = jnp.where(has_dn, norm(jnp.where(low, z4[i, ev, :], z4[i, od, :]), m_half), 0.0).astype(BF)
            row = lax.broadcasted_iota(jnp.int32, (half, 1), 0)

            def nxt(t):
                return jnp.where(row == half - 1, jnp.zeros_like(t), pltpu.roll(t, half - 1, 0))

            z = dot(cat([e, o, nxt(e), b4, nxt(b4)], 1), wd[...])
            zb[n] = z
            carry = add_stats(carry, z)
        return carry

    m = moments(1, lax.fori_loop(0, n_grp, stage_d, zero_stats), count_b, bn_down[...])

    def ex_copy(slot, g, src, dst, dev):
        part = pl.ds(g * GROUP, GROUP)
        return remote(src.at[1 - slot, part], dst.at[slot, part], ex_send.at[slot, g], ex_recv.at[slot, g], dev)

    def ex_start(g, src, dst):
        @pl.when(has_dn)
        def _():
            ex_copy(0, g, src, dst, dn).start()

        @pl.when(has_up)
        def _():
            ex_copy(1, g, src, dst, up).start()

    def ex_wait_send(src, dst):
        @pl.loop(0, n_grp)
        def _(g):
            @pl.when(has_dn)
            def _():
                ex_copy(0, g, src, dst, dn).wait_send()

            @pl.when(has_up)
            def _():
                ex_copy(1, g, src, dst, up).wait_send()

    def get(ref, part):
        return cat([ref[r, part].reshape(part.size * half, 128) for r in range(2)], 1)

    def put(ref, part, v):
        for r in range(2):
            ref[r, part] = v[:, r * 128:(r + 1) * 128].reshape(part.size, half, 128)

    def ex_batch(g, src, dst):
        for c in range(chunks):
            ex_start(g * chunks + c, src, dst)

    lane = lax.broadcasted_iota(jnp.int32, (1, 256), 1)
    valid = ((lane < 128) & has_up) | ((lane >= 128) & has_dn)

    for j in range(blocks):
        m_prev = m
        src, dst = (hb, hh) if j == 0 else (ub, rb)

        def conv_in(g, carry):
            part = pl.ds(g * BATCH, BATCH)
            z = zb[part].reshape(rows_b, 256)
            if j == 0:
                h = norm(z, m_prev).astype(BF)
            else:
                h = jnp.maximum((z - m_prev[0]) * m_prev[1] + m_prev[2] + get(hb, part).astype(F32), 0.0).astype(BF)
            put(hb, part, h)
            if j == 0:
                @pl.when(g > 0)
                def _():
                    ex_batch(g - 1, src, dst)
            z = dot(h, w_in[j])
            zb[part] = z.reshape(BATCH, half, 256)
            return add_stats(carry, z)

        stats = lax.fori_loop(0, n_bat, conv_in, zero_stats)
        if j == 0:
            ex_batch(n_bat - 1, src, dst)

        def halo_rows(g, many):
            part = pl.ds(g * GROUP * many, GROUP * many)
            for c in range(many):
                @pl.when(has_up)
                def _():
                    ex_copy(0, g * many + c, src, dst, dn).wait_recv()

                @pl.when(has_dn)
                def _():
                    ex_copy(1, g * many + c, src, dst, up).wait_recv()

            h = get(hh, part)
            if j > 0:
                z = dot(get(rb, part), w_out[j - 1])
                h = jnp.maximum((z - m_prev[0]) * m_prev[1] + m_prev[2] + h.astype(F32), 0.0).astype(BF)
                if j < blocks - 1:
                    put(hh, part, h)
            return dot(h, w_in[j])

        def taps(g, many, zh, carry):
            images = GROUP * many
            part = pl.ds(g * images, images)
            u = norm(zb[part].reshape(images * half, 256), m_in).astype(BF)
            z = dot(shifts(u, half), w_mid[j, :768])
            v = jnp.where(valid, norm(zh, m_in), 0.0).astype(BF)
            z = z + dot(shifts(v, half), w_mid[j, 768:])
            zb[part] = z.reshape(images, half, 256)
            return add_stats(carry, z)

        def conv_mid(g, carry, many):
            return taps(g, many, halo_rows(g, many), carry)

        def first_pair():
            @pl.loop(0, 2)
            def _(g):
                zh = halo_rows(g, 1)
                for c in range(2):
                    za[c, pl.ds(g * fold, fold)] = zh[:, c * 128:(c + 1) * 128].reshape(fold, width, 128)

        m_in = moments(2 + 3 * j, stats, count_b, bn_in[j], meanwhile=first_pair)

        def prepared(g, carry):
            zh = cat([za[c, pl.ds(g * fold, fold)].reshape(rows, 128) for c in range(2)], 1)
            return taps(g, 1, zh, carry)

        stats = lax.fori_loop(0, 2, prepared, zero_stats)

        stats = lax.fori_loop(1, n_grp // 2 - LATE, functools.partial(conv_mid, many=2), stats)
        stats = lax.fori_loop(n_grp - 2 * LATE, n_grp, functools.partial(conv_mid, many=1), stats)
        ex_wait_send(src, dst)
        m_mid = moments(3 + 3 * j, stats, count_b, bn_mid[j])

        def conv_out(g, carry):
            part = pl.ds(g * BATCH, BATCH)
            u = norm(zb[part].reshape(rows_b, 256), m_mid).astype(BF)
            if j < blocks - 1:
                put(ub, part, u)

                @pl.when(g > 0)
                def _():
                    ex_batch(g - 1, ub, rb)
            z = dot(u, w_out[j])
            zb[part] = z.reshape(BATCH, half, 256)
            return add_stats(carry, z)

        stats = lax.fori_loop(0, n_bat, conv_out, zero_stats)
        if j < blocks - 1:
            ex_batch(n_bat - 1, ub, rb)
        m = moments(4 + 3 * j, stats, count_b, bn_out[j])

    def finish(g, carry):
        part = pl.ds(g * BATCH, BATCH)
        z = zb[part].reshape(rows_b, 256)
        h = jnp.maximum((z - m[0]) * m[1] + m[2] + get(hb, part).astype(F32), 0.0).astype(BF)
        put(hb, part, h)
        return carry

    lax.fori_loop(0, n_bat, finish, 0)

    @pl.loop(0, n_grp)
    def _(g):
        @pl.when(has_dn)
        def _():
            img_copy(0, g, dn).wait_send()

        @pl.when(has_up)
        def _():
            img_copy(1, g, up).wait_send()
            img_copy(2, g, up).wait_send()

    for k in range(2 + 3 * blocks):
        if k in direct_ks:
            d = direct_ks.index(k)
            for i in range(1, sp_n):
                direct(d, lax.rem(me + i, sp_n)).wait_send()
            continue

        remote(msg.at[k], pslot.at[k], ar_send.at[k, 0], ar_recv.at[k, 3], me).wait_send()
        for c in range(2):
            remote(cmsg.at[k], slots.at[k, 0], ar_send.at[k, 1 + c], ar_recv.at[k, 0], me).wait_send()

        @pl.when(core == lax.rem(chip, 2))
        def _():
            for c in range(2):
                remote(cmsg.at[k], slots.at[k, 2], ar_send.at[k, 3 + c], ar_recv.at[k, 2], me).wait_send()


def solution(mesh):
    sp_n = mesh.shape["sp"]

    def forward(images, w_a, bn_a, w_down, bn_down, w_in, bn_in, w_mid, bn_mid, w_out, bn_out):
        n_img, rows_dev, width, chan = images.shape
        half = width // 2
        blocks = w_in.shape[0]
        n_bn = 2 + 3 * blocks
        n_grp = n_img // GROUP
        x = jnp.transpose(images, (0, 1, 3, 2))
        dims = (n_img, width, sp_n, blocks, n_img * rows_dev * width * sp_n, n_img * (rows_dev // 2) * half * sp_n)
        vmem = pl.BlockSpec(memory_space=pltpu.VMEM)
        anys = pl.BlockSpec(memory_space=pl.ANY)
        plane = (2, n_img, half, 128)
        rows_first = pl.pallas_call(
            functools.partial(body, dims),
            out_shape=pltpu.VMEM(plane, BF),
            in_specs=[anys] * 6 + [vmem] * 5,
            out_specs=vmem,
            scratch_shapes=[
                pltpu.VMEM(w_a.shape, BF),
                pltpu.VMEM(w_down.shape, BF),
                pltpu.VMEM(w_in.shape, BF),
                pltpu.VMEM(w_mid.shape, BF),
                pltpu.VMEM(w_out.shape, BF),
                pltpu.VMEM((1152, 256), BF),
                pltpu.VMEM((768, 128), BF),
                pltpu.VMEM((1024, 256), BF),
                pltpu.VMEM((blocks, 256, 256), BF),
                pltpu.VMEM((blocks, 256, 256), BF),
                pltpu.VMEM((blocks, 1536, 256), BF),
                pltpu.VMEM((2, GROUP, rows_dev, chan, width), BF),
                pltpu.VMEM((3, n_img, chan, width), BF),
                pltpu.VMEM((2, n_img, width, 128), F32),
                pltpu.VMEM((GROUP, width, 128), F32),
                pltpu.VMEM((n_img, half, 256), F32),
                pltpu.VMEM(plane, BF),
                pltpu.VMEM(plane, BF),
                pltpu.VMEM(plane, BF),
                pltpu.VMEM((n_bn, 8, 128), F32),
                pltpu.VMEM((n_bn, 8, 128), F32),
                pltpu.VMEM((n_bn, 8, 128), F32),
                pltpu.VMEM((n_bn, 3, 8, 128), F32),
                pltpu.SemaphoreType.DMA((2,)),
                pltpu.SemaphoreType.DMA((3, n_grp)),
                pltpu.SemaphoreType.DMA((3, n_grp)),
                pltpu.SemaphoreType.DMA((2, n_grp)),
                pltpu.SemaphoreType.DMA((2, n_grp)),
                pltpu.SemaphoreType.DMA((n_bn, 5)),
                pltpu.SemaphoreType.DMA((n_bn, 4)),
                pltpu.SemaphoreType.DMA((5,)),
                pltpu.VMEM((2 + blocks, sp_n, 8, 128), F32),
                pltpu.SemaphoreType.DMA((2 + blocks, sp_n)),
                pltpu.SemaphoreType.DMA((2 + blocks, sp_n)),
            ],
            compiler_params=pltpu.CompilerParams(
                collective_id=0, has_side_effects=True, vmem_limit_bytes=67043328 - 2 * n_img * half * 128 * 2),
            name="stack",
        )(x, w_a, w_down, w_in, w_mid, w_out, bn_a, bn_down, bn_in, bn_mid, bn_out)
        return jnp.transpose(rows_first, (1, 0, 2, 3))

    act_spec = P("dp", "sp", None, None)
    return jax.shard_map(forward, mesh=mesh, in_specs=(act_spec,) + (P(),) * 10, out_specs=act_spec, check_vma=False)
```

```python
import functools

import jax
import jax.numpy as jnp
from jax import lax
from jax.experimental import pallas as pl
from jax.experimental.pallas import tpu as pltpu
from jax.sharding import PartitionSpec as P

NORM_EPS = 1e-5
BF = jnp.bfloat16
F32 = jnp.float32
GROUP = 4
LATE = 1
BATCH = 8


def cat(parts, axis):
    return jnp.concatenate(parts, axis=axis)


def banded(taps, rows_in, rows_out, stride, first):
    zero = jnp.zeros_like(taps[0])
    rows = []
    for ri in rows_in:
        cols = []
        for ro in rows_out:
            dy = ri + first - stride * ro
            cols.append(taps[dy] if 0 <= dy < len(taps) else zero)
        rows.append(cat(cols, 1))
    return cat(rows, 0)


def pack_stage_a(w_a, w_down, wa, w4, wd):
    for dx in range(3):
        ta = [w_a[0, dy, dx] for dy in range(3)]
        zero = jnp.zeros_like(ta[0])
        wa[pl.ds(dx * 384, 384)] = banded(ta, range(6), range(4), 1, 0)
        w4[pl.ds(dx * 256, 256)] = cat([cat([t, t], 1) for t in ta + [zero]], 0)
        td = [w_down[dy, dx] for dy in range(3)]
        wd[pl.ds(dx * 256, 256)] = banded(td, range(4), range(2), 2, 0)
        none = jnp.zeros_like(td[2])
        wd[pl.ds(768 + dx * 64, 64)] = cat([none, td[2]], 1)
    wd[pl.ds(960, 64)] = jnp.zeros((64, 256), BF)


def pack_stage_b(w_in, w_mid, w_out, in2, out2, mid2):
    def diag(a, b):
        z = jnp.zeros_like(a)
        return cat([cat([a, z], 1), cat([z, b], 1)], 0)

    for j in range(w_in.shape[0]):
        in2[j] = diag(w_in[j], w_in[j])
        out2[j] = diag(w_out[j], w_out[j])
        for dx in range(3):
            tm = [w_mid[j, dy, dx] for dy in range(3)]
            mid2[j, pl.ds(dx * 256, 256)] = banded(tm, (0, 1), (0, 1), 1, 1)
            mid2[j, pl.ds(768 + dx * 256, 256)] = diag(tm[0], tm[2])


def body(
    dims, img, w_a_hbm, w_down_hbm, w_in_hbm, w_mid_hbm, w_out_hbm, bn_a, bn_down, bn_in, bn_mid, bn_out, hb,
    w_a_raw, w_down_raw, w_in_raw, w_mid_raw, w_out_raw, wa, w4, wd, w_in, w_out, w_mid,
    xb, halo, za, z4, zb, ub, hh, rb,
    msg, pslot, cmsg, slots,
    ld_sem, im_send, im_recv, ex_send, ex_recv, ar_send, ar_recv, w_sem, all8, d_send, d_recv,
):
    n_img, width, sp_n, blocks, count_a, count_b = dims
    half = width // 2
    n_grp = n_img // GROUP
    rows = GROUP * half
    fold = rows // width
    n_bat = n_img // BATCH
    rows_b = BATCH * half
    chunks = BATCH // GROUP
    me = lax.axis_index("sp")
    core = lax.rem(me, 2)
    chip = lax.div(me, 2)
    chips = sp_n // 2
    has_up = me > 0
    has_dn = me < sp_n - 1
    up = jnp.maximum(me - 1, 0)
    dn = jnp.minimum(me + 1, sp_n - 1)

    def remote(src, dst, ssem, rsem, dev):
        return pltpu.make_async_remote_copy(
            src_ref=src, dst_ref=dst, send_sem=ssem, recv_sem=rsem,
            device_id={"sp": dev}, device_id_type=pl.DeviceIdType.MESH)

    w_copies = [
        pltpu.make_async_copy(src, dst, w_sem.at[i]) for i, (src, dst) in enumerate((
            (w_a_hbm, w_a_raw), (w_down_hbm, w_down_raw), (w_in_hbm, w_in_raw), (w_mid_hbm, w_mid_raw), (w_out_hbm, w_out_raw)))]
    for copy in w_copies:
        copy.start()

    def load(g):
        slot = lax.rem(g, 2)
        return pltpu.make_async_copy(img.at[pl.ds(g * GROUP, GROUP)], xb.at[slot], ld_sem.at[slot])

    load(0).start()

    direct_ks = [1] + [3 + 3 * j for j in range(blocks)] + [1 + 3 * blocks]

    bar = pltpu.get_barrier_semaphore()
    for k in range(1, sp_n):
        pl.semaphore_signal(bar, inc=1, device_id={"sp": lax.rem(me + k, sp_n)}, device_id_type=pl.DeviceIdType.MESH)
    pl.semaphore_wait(bar, sp_n - 1)

    def img_copy(slot, g, dev):
        row = (3, 0, 1)[slot]
        part = pl.ds(g * GROUP, GROUP)
        return remote(img.at[part, row], halo.at[slot, part], im_send.at[slot, g], im_recv.at[slot, g], dev)

    @pl.loop(0, n_grp)
    def _(g):
        @pl.when(has_dn)
        def _():
            img_copy(0, g, dn).start()

        @pl.when(has_up)
        def _():
            img_copy(1, g, up).start()

    @pl.when(has_up)
    def _():
        @pl.loop(0, n_grp)
        def _(g):
            img_copy(2, g, up).start()

    @pl.when(jnp.logical_not(has_up))
    def _():
        @pl.loop(0, n_img)
        def _(n):
            halo[0, n] = jnp.zeros(halo.shape[2:], BF)
            hh[0, n] = jnp.zeros(hh.shape[2:], BF)
            rb[0, n] = jnp.zeros(rb.shape[2:], BF)

    @pl.when(jnp.logical_not(has_dn))
    def _():
        @pl.loop(0, n_img)
        def _(n):
            halo[1, n] = jnp.zeros(halo.shape[2:], BF)
            halo[2, n] = jnp.zeros(halo.shape[2:], BF)
            hh[1, n] = jnp.zeros(hh.shape[2:], BF)
            rb[1, n] = jnp.zeros(rb.shape[2:], BF)

    def dot(a, b):
        return jnp.dot(a, b, preferred_element_type=F32)

    def add_stats(carry, z):
        s, q = carry
        zz = z.reshape(z.shape[0] // 8, 8, z.shape[1])
        return s + jnp.sum(zz, axis=0), q + jnp.sum(zz * zz, axis=0)

    zero_stats = (jnp.zeros((8, 256), F32), jnp.zeros((8, 256), F32))

    def norm(z, m):
        return jnp.maximum((z - m[0]) * m[1] + m[2], 0.0)

    def direct(d, other):
        return remote(msg.at[direct_ks[d]], all8.at[d, me], d_send.at[d, other], d_recv.at[d, me], other)

    def moments(k, stats, count, p, fold64=False, meanwhile=None):
        s, q = (t[:, :128] + t[:, 128:] for t in stats)
        if fold64:
            s, q = s + pltpu.roll(s, 64, 1), q + pltpu.roll(q, 64, 1)
        own = cat([jnp.sum(s, axis=0, keepdims=True), jnp.sum(q, axis=0, keepdims=True), jnp.zeros((6, 128), F32)], 0)
        msg[k] = own
        if k in direct_ks:
            d = direct_ks.index(k)
            all8[d, me] = own
            for i in sorted(range(1, sp_n), key=lambda i: abs(i - chips)):
                direct(d, lax.rem(me + i, sp_n)).start()
            for i in range(1, sp_n):
                other = lax.rem(me + i, sp_n)
                remote(msg.at[k], all8.at[d, other], d_send.at[d, other], d_recv.at[d, other], other).wait_recv()
            parts = [all8[d, i] for i in range(sp_n)]
            while len(parts) > 1:
                parts = [parts[i] + parts[i + 1] for i in range(0, len(parts), 2)]
            tot = parts[0]
        else:
            first = remote(msg.at[k], pslot.at[k], ar_send.at[k, 0], ar_recv.at[k, 3], me + 1 - 2 * core)
            first.start()
            first.wait_recv()
            mine = own + pslot[k]
            cmsg[k] = mine
            near = lax.rem(chip + 1 + core * (chips - 2), chips)
            far = lax.rem(chip + 2, chips)
            @pl.when(core == lax.rem(chip, 2))
            def _():
                for c in range(2):
                    remote(cmsg.at[k], slots.at[k, 2], ar_send.at[k, 3 + c], ar_recv.at[k, 2], far * 2 + c).start()

            for c in range(2):
                remote(cmsg.at[k], slots.at[k, core], ar_send.at[k, 1 + c], ar_recv.at[k, core], near * 2 + c).start()

            if meanwhile is not None:
                meanwhile()
            for c in range(3):
                remote(cmsg.at[k], slots.at[k, c], ar_send.at[k, 1], ar_recv.at[k, c], me).wait_recv()
            tot = (mine + slots[k, 2]) + (slots[k, 0] + slots[k, 1])
        inv = 1.0 / count
        mean = tot[0:1] * inv
        var = tot[1:2] * inv - mean * mean
        scale = p[0:1] * lax.rsqrt(var + NORM_EPS)
        return tuple(cat([t, t], 1) for t in (mean, scale, p[1:2]))

    def shifts(u, line):
        row = lax.rem(lax.broadcasted_iota(jnp.int32, (u.shape[0], 1), 0), line)
        zero = jnp.zeros_like(u)
        prev = jnp.where(row == 0, zero, pltpu.roll(u, 1, 0))
        nxt = jnp.where(row == line - 1, zero, pltpu.roll(u, u.shape[0] - 1, 0))
        return cat([prev, u, nxt], 1)

    for copy in w_copies:
        copy.wait()
    pack_stage_a(w_a_raw, w_down_raw, wa, w4, wd)
    pack_stage_b(w_in_raw, w_mid_raw, w_out_raw, w_in, w_out, w_mid)

    def stage_a(g, carry):
        @pl.when(g + 1 < n_grp)
        def _():
            load(g + 1).start()

        @pl.when(has_up)
        def _():
            img_copy(0, g, dn).wait_recv()

        @pl.when(has_dn)
        def _():
            img_copy(1, g, up).wait_recv()

        load(g).wait()
        for i in range(GROUP):
            n = g * GROUP + i
            x = xb.at[lax.rem(g, 2), i]
            t0 = cat([halo[0, n], x[0]], 0).T
            t1 = cat([x[1], x[2]], 0).T
            t2 = cat([x[3], halo[1, n]], 0).T
            hb[0, n] = t2[:half]
            hb[1, n] = t2[half:]
            z = dot(shifts(cat([t0, t1, t2], 1), width), wa[...])
            za[0, n] = z[:, :128]
            za[1, n] = z[:, 128:]
            carry = add_stats(carry, z)
        return carry

    m = moments(0, lax.fori_loop(0, n_grp, stage_a, zero_stats), count_a, cat([bn_a[0], bn_a[0]], 1), True)
    m_half = tuple(t[:, :128] for t in m)

    low = lax.broadcasted_iota(jnp.int32, (1, 128), 1) < 64

    def stage_d(g, carry):
        @pl.when(has_dn)
        def _():
            img_copy(2, g, up).wait_recv()

        for i in range(GROUP):
            n = g * GROUP + i
            t2 = cat([hb[0, n], hb[1, n]], 0)
            t3 = cat([halo[2, n], halo[2, n]], 0).T
            z4[i] = dot(shifts(cat([t2, t3], 1), width), w4[...])
        for i in range(GROUP):
            n = g * GROUP + i
            ev, od = pl.ds(0, half, stride=2), pl.ds(1, half, stride=2)
            e = norm(cat([za[0, n, ev, :], za[1, n, ev, :]], 1), m).astype(BF)
            o = norm(cat([za[0, n, od, :], za[1, n, od, :]], 1), m).astype(BF)
            b4 = jnp.where(has_dn, norm(jnp.where(low, z4[i, ev, :], z4[i, od, :]), m_half), 0.0).astype(BF)
            row = lax.broadcasted_iota(jnp.int32, (half, 1), 0)

            def nxt(t):
                return jnp.where(row == half - 1, jnp.zeros_like(t), pltpu.roll(t, half - 1, 0))

            z = dot(cat([e, o, nxt(e), b4, nxt(b4)], 1), wd[...])
            zb[n] = z
            carry = add_stats(carry, z)
        return carry

    m = moments(1, lax.fori_loop(0, n_grp, stage_d, zero_stats), count_b, bn_down[...])

    def ex_copy(slot, g, src, dst, dev):
        part = pl.ds(g * GROUP, GROUP)
        return remote(src.at[1 - slot, part], dst.at[slot, part], ex_send.at[slot, g], ex_recv.at[slot, g], dev)

    def ex_start(g, src, dst):
        @pl.when(has_dn)
        def _():
            ex_copy(0, g, src, dst, dn).start()

        @pl.when(has_up)
        def _():
            ex_copy(1, g, src, dst, up).start()

    def ex_wait_send(src, dst):
        @pl.loop(0, n_grp)
        def _(g):
            @pl.when(has_dn)
            def _():
                ex_copy(0, g, src, dst, dn).wait_send()

            @pl.when(has_up)
            def _():
                ex_copy(1, g, src, dst, up).wait_send()

    def get(ref, part):
        return cat([ref[r, part].reshape(part.size * half, 128) for r in range(2)], 1)

    def put(ref, part, v):
        for r in range(2):
            ref[r, part] = v[:, r * 128:(r + 1) * 128].reshape(part.size, half, 128)

    def ex_batch(g, src, dst):
        for c in range(chunks):
            ex_start(g * chunks + c, src, dst)

    lane = lax.broadcasted_iota(jnp.int32, (1, 256), 1)
    valid = ((lane < 128) & has_up) | ((lane >= 128) & has_dn)

    for j in range(blocks):
        m_prev = m
        src, dst = (hb, hh) if j == 0 else (ub, rb)

        batch = GROUP if j == 0 else BATCH

        def conv_in(g, carry):
            part = pl.ds(g * batch, batch)
            z = zb[part].reshape(batch * half, 256)
            if j == 0:
                h = norm(z, m_prev).astype(BF)
            else:
                h = jnp.maximum((z - m_prev[0]) * m_prev[1] + m_prev[2] + get(hb, part).astype(F32), 0.0).astype(BF)
            put(hb, part, h)
            if j == 0:
                @pl.when(g > 0)
                def _():
                    ex_start(g - 1, src, dst)
            z = dot(h, w_in[j])
            zb[part] = z.reshape(batch, half, 256)
            return add_stats(carry, z)

        stats = lax.fori_loop(0, n_img // batch, conv_in, zero_stats)
        if j == 0:
            ex_start(n_grp - 1, src, dst)

        def halo_rows(g, many):
            part = pl.ds(g * GROUP * many, GROUP * many)
            for c in range(many):
                @pl.when(has_up)
                def _():
                    ex_copy(0, g * many + c, src, dst, dn).wait_recv()

                @pl.when(has_dn)
                def _():
                    ex_copy(1, g * many + c, src, dst, up).wait_recv()

            h = get(hh, part)
            if j > 0:
                z = dot(get(rb, part), w_out[j - 1])
                h = jnp.maximum((z - m_prev[0]) * m_prev[1] + m_prev[2] + h.astype(F32), 0.0).astype(BF)
                if j < blocks - 1:
                    put(hh, part, h)
            return dot(h, w_in[j])

        def taps(g, many, zh, carry):
            images = GROUP * many
            part = pl.ds(g * images, images)
            u = norm(zb[part].reshape(images * half, 256), m_in).astype(BF)
            z = dot(shifts(u, half), w_mid[j, :768])
            v = jnp.where(valid, norm(zh, m_in), 0.0).astype(BF)
            z = z + dot(shifts(v, half), w_mid[j, 768:])
            zb[part] = z.reshape(images, half, 256)
            return add_stats(carry, z)

        def conv_mid(g, carry, many):
            return taps(g, many, halo_rows(g, many), carry)

        def first_pair():
            @pl.loop(0, 2)
            def _(g):
                zh = halo_rows(g, 1)
                for c in range(2):
                    za[c, pl.ds(g * fold, fold)] = zh[:, c * 128:(c + 1) * 128].reshape(fold, width, 128)

        m_in = moments(2 + 3 * j, stats, count_b, bn_in[j], meanwhile=first_pair)

        def prepared(g, carry):
            zh = cat([za[c, pl.ds(g * fold, fold)].reshape(rows, 128) for c in range(2)], 1)
            return taps(g, 1, zh, carry)

        stats = lax.fori_loop(0, 2, prepared, zero_stats)

        stats = lax.fori_loop(1, n_grp // 2 - LATE, functools.partial(conv_mid, many=2), stats)
        stats = lax.fori_loop(n_grp - 2 * LATE, n_grp, functools.partial(conv_mid, many=1), stats)
        ex_wait_send(src, dst)
        m_mid = moments(3 + 3 * j, stats, count_b, bn_mid[j])

        def conv_out(g, carry):
            part = pl.ds(g * BATCH, BATCH)
            u = norm(zb[part].reshape(rows_b, 256), m_mid).astype(BF)
            if j < blocks - 1:
                put(ub, part, u)

                @pl.when(g > 0)
                def _():
                    ex_batch(g - 1, ub, rb)
            z = dot(u, w_out[j])
            zb[part] = z.reshape(BATCH, half, 256)
            return add_stats(carry, z)

        stats = lax.fori_loop(0, n_bat, conv_out, zero_stats)
        if j < blocks - 1:
            ex_batch(n_bat - 1, ub, rb)
        m = moments(4 + 3 * j, stats, count_b, bn_out[j])

    def finish(g, carry):
        part = pl.ds(g * BATCH, BATCH)
        z = zb[part].reshape(rows_b, 256)
        h = jnp.maximum((z - m[0]) * m[1] + m[2] + get(hb, part).astype(F32), 0.0).astype(BF)
        put(hb, part, h)
        return carry

    lax.fori_loop(0, n_bat, finish, 0)

    @pl.loop(0, n_grp)
    def _(g):
        @pl.when(has_dn)
        def _():
            img_copy(0, g, dn).wait_send()

        @pl.when(has_up)
        def _():
            img_copy(1, g, up).wait_send()
            img_copy(2, g, up).wait_send()

    for k in range(2 + 3 * blocks):
        if k in direct_ks:
            d = direct_ks.index(k)
            for i in range(1, sp_n):
                direct(d, lax.rem(me + i, sp_n)).wait_send()
            continue

        remote(msg.at[k], pslot.at[k], ar_send.at[k, 0], ar_recv.at[k, 3], me).wait_send()
        for c in range(2):
            remote(cmsg.at[k], slots.at[k, 0], ar_send.at[k, 1 + c], ar_recv.at[k, 0], me).wait_send()

        @pl.when(core == lax.rem(chip, 2))
        def _():
            for c in range(2):
                remote(cmsg.at[k], slots.at[k, 2], ar_send.at[k, 3 + c], ar_recv.at[k, 2], me).wait_send()


def solution(mesh):
    sp_n = mesh.shape["sp"]

    def forward(images, w_a, bn_a, w_down, bn_down, w_in, bn_in, w_mid, bn_mid, w_out, bn_out):
        n_img, rows_dev, width, chan = images.shape
        half = width // 2
        blocks = w_in.shape[0]
        n_bn = 2 + 3 * blocks
        n_grp = n_img // GROUP
        x = jnp.transpose(images, (0, 1, 3, 2))
        dims = (n_img, width, sp_n, blocks, n_img * rows_dev * width * sp_n, n_img * (rows_dev // 2) * half * sp_n)
        vmem = pl.BlockSpec(memory_space=pltpu.VMEM)
        anys = pl.BlockSpec(memory_space=pl.ANY)
        plane = (2, n_img, half, 128)
        rows_first = pl.pallas_call(
            functools.partial(body, dims),
            out_shape=pltpu.VMEM(plane, BF),
            in_specs=[anys] * 6 + [vmem] * 5,
            out_specs=vmem,
            scratch_shapes=[
                pltpu.VMEM(w_a.shape, BF),
                pltpu.VMEM(w_down.shape, BF),
                pltpu.VMEM(w_in.shape, BF),
                pltpu.VMEM(w_mid.shape, BF),
                pltpu.VMEM(w_out.shape, BF),
                pltpu.VMEM((1152, 256), BF),
                pltpu.VMEM((768, 128), BF),
                pltpu.VMEM((1024, 256), BF),
                pltpu.VMEM((blocks, 256, 256), BF),
                pltpu.VMEM((blocks, 256, 256), BF),
                pltpu.VMEM((blocks, 1536, 256), BF),
                pltpu.VMEM((2, GROUP, rows_dev, chan, width), BF),
                pltpu.VMEM((3, n_img, chan, width), BF),
                pltpu.VMEM((2, n_img, width, 128), F32),
                pltpu.VMEM((GROUP, width, 128), F32),
                pltpu.VMEM((n_img, half, 256), F32),
                pltpu.VMEM(plane, BF),
                pltpu.VMEM(plane, BF),
                pltpu.VMEM(plane, BF),
                pltpu.VMEM((n_bn, 8, 128), F32),
                pltpu.VMEM((n_bn, 8, 128), F32),
                pltpu.VMEM((n_bn, 8, 128), F32),
                pltpu.VMEM((n_bn, 3, 8, 128), F32),
                pltpu.SemaphoreType.DMA((2,)),
                pltpu.SemaphoreType.DMA((3, n_grp)),
                pltpu.SemaphoreType.DMA((3, n_grp)),
                pltpu.SemaphoreType.DMA((2, n_grp)),
                pltpu.SemaphoreType.DMA((2, n_grp)),
                pltpu.SemaphoreType.DMA((n_bn, 5)),
                pltpu.SemaphoreType.DMA((n_bn, 4)),
                pltpu.SemaphoreType.DMA((5,)),
                pltpu.VMEM((2 + blocks, sp_n, 8, 128), F32),
                pltpu.SemaphoreType.DMA((2 + blocks, sp_n)),
                pltpu.SemaphoreType.DMA((2 + blocks, sp_n)),
            ],
            compiler_params=pltpu.CompilerParams(
                collective_id=0, has_side_effects=True, vmem_limit_bytes=67043328 - 2 * n_img * half * 128 * 2),
            name="stack",
        )(x, w_a, w_down, w_in, w_mid, w_out, bn_a, bn_down, bn_in, bn_mid, bn_out)
        return jnp.transpose(rows_first, (1, 0, 2, 3))

    act_spec = P("dp", "sp", None, None)
    return jax.shard_map(forward, mesh=mesh, in_specs=(act_spec,) + (P(),) * 10, out_specs=act_spec, check_vma=False)
```
